128 devices in a mesh: freq: 8 (over y, core), mesh: 16 (over z, x).
Axes of the slice: x: 4, y: 4, z: 4, core: 2. Of those that a mesh axis runs over, the one named last changes fastest.
Arguments:
- spectrum: float32 [2, 216, 65536], P(None, 'freq', 'mesh'), may hold values from -84 to 84
- time_weights: float32 [2, 432], P(None, 'freq'), may hold values from -0.875 to 0.875
- interp_weights: float32 [2048, 128, 128], P('mesh'), may hold values from -0.5 to 0.5
- group_block: int32 [2048], P('mesh'), may hold values from 0 to 511, as said below
- group_count: int32 [16], P('mesh'), may hold values from 64 to 128, as said below
- wave_state: float32 [8, 2, 1048576], P('freq', None, 'mesh'), may hold values from -6 to 6
- neighbors: int32 [4, 8192], P(None, 'mesh'), may hold values from 0 to 575, as said below
- coupling: float32 [4, 1048576], P(None, 'mesh'), may hold values from 0.02 to 0.2
Outputs:
- series: float32 [432, 65536], P('freq', 'mesh')
- new_state: float32 [8, 2, 1048576], P('freq', None, 'mesh')
The draws below stay inside these ranges and needn't reach their ends.
Inputs may be any that keep to these rules, and one draw needn't show every extreme that they name: `group_block`: partition o owns blocks o * 32 to o * 32 + 31. Of one partition's 128 groups at most 8 name blocks of one owner, and each partition has an owner named by exactly 8 of its live groups. The live groups of partition m are its first group_count[m]; some partition has exactly 128. `neighbors`: for the cell row with local row index u, a value e names local row e - 32 of the row's own partition when it lies in 32 .. (69632) // 128 - 1, else a row of the neighbouring partition below or above; never the row itself.
All inputs are finite; a program needn't handle non-finite values.
Results may differ from the reference program's by a relative error of at most 0.0001.
Values sent between devices are 32-bit elements; how exact they have to be, the bound alone decides.
A program may use at most 64 MiB of HBM per device.

```python
import math
import jax
import jax.numpy as jnp
from jax import lax

NF = 216
NT = 432
BS = 128
B_DEV = 32
NB = 512
NP = 65536
FG_MAX = 128
GROUPS = 2048
C_DEV = 65536
CELLS = 1048576
LANES = 128
HB = 4096
NEIGH = 4
WINDOWS = 8
N_FREQ = 8
N_MESH = 16


def group_plan(base_key):
    count_key = jax.random.fold_in(base_key, 7)
    heaviest = jax.random.randint(jax.random.fold_in(count_key, 1), (), 0, N_MESH)
    lighter = jax.random.randint(jax.random.fold_in(count_key, 2), (N_MESH,), FG_MAX // 2, FG_MAX + 1)
    partitions = jnp.arange(N_MESH, dtype=jnp.int32)
    counts = jnp.where(partitions == heaviest, FG_MAX, lighter).astype(jnp.int32)
    capacity = max(2, FG_MAX // N_MESH)

    def one_partition(partition, live_count):
        partition_key = jax.random.fold_in(base_key, 1000 + partition)
        leading = jax.random.randint(jax.random.fold_in(partition_key, 1), (), 0, N_MESH).astype(jnp.int32)
        others = jax.random.permutation(jax.random.fold_in(partition_key, 2), (N_MESH - 1) * capacity) // capacity
        others = jnp.where(others >= leading, others + 1, others).astype(jnp.int32)
        owners = jnp.concatenate([jnp.full((capacity,), leading, jnp.int32), others])[:FG_MAX]
        positions = jnp.arange(FG_MAX, dtype=jnp.int32)
        ranking = jax.random.permutation(jax.random.fold_in(partition_key, 3), FG_MAX).astype(jnp.int32)
        scores = jnp.where(positions < live_count, ranking, FG_MAX + positions)
        ordering = jnp.argsort(scores, stable=True)
        owners = owners[ordering]
        inside = jax.random.randint(jax.random.fold_in(partition_key, 4), (FG_MAX,), 0, B_DEV)
        return (owners * B_DEV + inside).astype(jnp.int32)
    blocks = jax.vmap(one_partition)(partitions, counts)
    return (blocks.reshape(N_MESH * FG_MAX), counts)


def draw_group_block(key, part):
    return group_plan(key)[0]


def draw_group_count(key, part):
    return group_plan(key)[1]


def draw_neighbors(key, part):
    halo_rows = HB // LANES
    rows_local = C_DEV // LANES
    local_rows = jnp.arange(CELLS // LANES, dtype=jnp.int32) % rows_local
    offsets = jax.random.randint(jax.random.fold_in(key, 21), (NEIGH, CELLS // LANES), -halo_rows, halo_rows)
    offsets = jnp.where(offsets >= 0, offsets + 1, offsets)
    return (halo_rows + local_rows[None, :] + offsets).astype(jnp.int32)


def block_scale(key, shape, pieces, smallest, largest):
    gain, own = 1.0, jax.random.fold_in(key, 6)
    for dim, parts in pieces:
        heights = jnp.exp(jax.random.uniform(jax.random.fold_in(own, dim), (parts,), jnp.float32, smallest / len(pieces), largest / len(pieces)))
        gain = gain * jnp.repeat(heights, shape[dim] // parts).reshape([-1 if axis == dim else 1 for axis in range(len(shape))])
    return gain


def normal_values(own_key, extent, scale, bound, cuts=(), kind=jnp.bfloat16):
    result = scale * jax.random.normal(own_key, extent, jnp.float32)
    if cuts:
        result = result * block_scale(own_key, extent, cuts, -0.22, 0.18)
    return jnp.clip(result, -bound, bound).astype(kind)


def setup_inputs(seed: int = 0) -> dict:
    seeds = jax.random.split(jax.random.key(seed), 9)
    spectrum = normal_values(seeds[0], (2, NF, NP), 14.0, 84.0, ((1, 8), (2, 16)), jnp.float32)
    time_weights = normal_values(seeds[1], (2, NT), (NT // N_FREQ) ** -0.5, 0.875, ((1, 8),), jnp.float32)
    interp_weights = normal_values(seeds[2], (GROUPS, BS, BS), BS ** -0.5, 0.5, ((0, 16),), jnp.float32)
    group_block = draw_group_block(jax.random.fold_in(seeds[8], 71), 0)
    group_count = draw_group_count(jax.random.fold_in(seeds[8], 71), 0)
    wave_state = normal_values(seeds[5], (WINDOWS, 2, CELLS), 1.0, 6.0, ((0, 8), (2, 16)), jnp.float32)
    neighbors = draw_neighbors(jax.random.fold_in(seeds[8], 71), 0)
    coupling = jnp.clip(jnp.exp(math.log(0.2) - 2.3025851 * jax.random.uniform(seeds[7], (NEIGH, CELLS), jnp.float32) ** block_scale(seeds[7], (NEIGH, CELLS), ((1, 16),), -0.2, 0.2)), 0.02, 0.2)
    return dict(spectrum=spectrum, time_weights=time_weights, interp_weights=interp_weights, group_block=group_block, group_count=group_count, wave_state=wave_state, neighbors=neighbors, coupling=coupling)


highest = lax.Precision.HIGHEST


def advance(previous, current, forcing, neighbors, coupling):
    halo_rows = HB // LANES
    row_count = CELLS // LANES
    rows_local = C_DEV // LANES
    cell_rows = current.reshape(row_count, LANES)
    extended = jnp.pad(cell_rows, ((halo_rows, halo_rows), (0, 0)))
    offsets = (jnp.arange(row_count, dtype=jnp.int32) // rows_local) * rows_local
    beside_all = extended[offsets[None, :] + neighbors].reshape(NEIGH, CELLS)
    spread = jnp.sum(coupling * (beside_all - current[None, :]), axis=0)
    return 2.0 * current - previous + spread + forcing


def reference(spectrum, time_weights, interp_weights, group_block, group_count, wave_state, neighbors, coupling):
    time_horizon = 2 * NF
    sample_times = jnp.arange(time_horizon, dtype=jnp.int32)
    angular_frequency = jnp.arange(NF, dtype=jnp.int32)
    phase_angles = ((sample_times[:, None] * angular_frequency[None, :]) % time_horizon).astype(jnp.float32)
    angles = phase_angles * (2.0 * math.pi / time_horizon)
    scales = jnp.where(angular_frequency == 0, 1.0, 2.0).astype(jnp.float32) / time_horizon
    basis_row_matrix = jnp.concatenate([jnp.cos(angles) * scales, -jnp.sin(angles) * scales], axis=1)
    series = jnp.dot(basis_row_matrix, spectrum.reshape(2 * NF, NP), precision=highest, preferred_element_type=jnp.float32)
    taper_window = time_horizon // N_FREQ
    live_mask = (jnp.arange(FG_MAX, dtype=jnp.int32)[None, :] < group_count[:, None]).reshape(GROUPS).astype(jnp.float32)
    blocks = series.reshape(time_horizon, NB, BS)
    states = []
    for window_index in range(N_FREQ):
        picked = blocks[window_index * taper_window:(window_index + 1) * taper_window][:, group_block, :]
        interpolated = jnp.einsum("rgp,gfp->rgf", picked, interp_weights, precision=highest)
        interpolated = interpolated * live_mask[None, :, None]
        weights_here = time_weights[:, window_index * taper_window:(window_index + 1) * taper_window]
        forcing = jnp.einsum("sr,rgf->sgf", weights_here, interpolated, precision=highest)
        forcing = forcing.reshape(2, N_MESH, FG_MAX * BS)
        forcing = jnp.pad(forcing, ((0, 0), (0, 0), (0, C_DEV - FG_MAX * BS))).reshape(2, CELLS)
        previous = wave_state[window_index, 0]
        current = wave_state[window_index, 1]
        stepped = advance(previous, current, forcing[0], neighbors, coupling)
        stepped_again = advance(current, stepped, forcing[1], neighbors, coupling)
        states.append(jnp.stack([stepped, stepped_again]))
    return series, jnp.stack(states)
```

```python
import math

import jax
import jax.numpy as jnp
import numpy as np
from jax import lax
from jax.experimental import pallas as pl
from jax.experimental.pallas import tpu as pltpu
from jax.sharding import PartitionSpec as P

MESH = pl.DeviceIdType.MESH
F32 = jnp.float32
BF16 = jnp.bfloat16

NF = 216
NT = 432
FD = 8
MD = 16
FL = NF // FD
TL = NT // FD
KP = 56
NP = 4096
COLS = NP // FD
HALVES = 2
HC = COLS // HALVES
BLK = 128
NBLK = NP // BLK
GROUPS = 128
ROWS = 512
HALO = 32
EXT = 640


def split_bf16(x):
    hi = x.astype(BF16)
    lo = (x - hi.astype(F32)).astype(BF16)
    return hi, lo


def host_split(x):
    hi = np.asarray(x, np.float32).astype(jnp.bfloat16)
    lo = (x - hi.astype(np.float64)).astype(jnp.bfloat16)
    return hi, lo


def host_basis():
    t = np.arange(NT)[:, None]
    k = np.arange(NF)[None, :]
    angle = (t * k % NT) * (2.0 * math.pi / NT)
    scale = np.where(k == 0, 1.0, 2.0) / NT
    full = np.zeros((FD, KP, FD, KP))
    full[:, :TL, :, :FL] = (np.cos(angle) * scale).reshape(FD, TL, FD, FL)
    full[:, :TL, :, FL : 2 * FL] = (-np.sin(angle) * scale).reshape(FD, TL, FD, FL)
    basis = np.stack(host_split(full.reshape(FD * KP, FD * KP)))
    own = np.zeros((FD, 64, FD, 64))
    own[:, :KP, :, :KP] = full.transpose(2, 1, 0, 3)
    own = own.reshape(FD, 64, FD * 64)
    return basis, np.stack(host_split(own), axis=1)


def dot(a, b):
    return jnp.dot(a, b, preferred_element_type=F32)


def dot_t(a, b):
    return lax.dot_general(a, b, (((1,), (1,)), ((), ())), preferred_element_type=F32)


def kernel(
    spec_h, tw_h, w_h, gb_h, gc_h, ws_h, nb_h, cp_h, basis_h, own_h,
    series_o, state_o,
    xs, xp, tws, twr, twf, cb, basis, r, s2, pb, ra, wsum, ag, wf, whl, oh, ws, cp, nb, gb, gc,
    hs, hcur, hb1, hpush, hps, sb, base1, base2, ns, lh, ee,
    lsem, tw_s, tw_r, x_s, x_r, a_s, a_r, g_s, g_r, h_s, h_r, y_s, y_r, mesh_sem,
):
    f = lax.axis_index("freq")
    m = lax.axis_index("mesh")
    z, x = m // 4, m % 4

    def fdev(d):
        return (lax.rem(f + d, FD), m)

    def mdev(d):
        return (f, lax.rem(m + d, MD))

    def remote(src, dst, ssem, rsem, dev):
        return pltpu.make_async_remote_copy(
            src_ref=src, dst_ref=dst, send_sem=ssem, recv_sem=rsem, device_id=dev, device_id_type=MESH
        )

    bar = pltpu.get_barrier_semaphore()
    xline = [(f, z * 4 + lax.rem(x + d, 4)) for d in range(1, 4)]
    zline = [(f, lax.rem(z + d, 4) * 4 + x) for d in range(1, 4)]
    first = [fdev(d) for d in range(1, FD)] + xline + zline
    for dev in first:
        pl.semaphore_signal(bar, inc=1, device_id=dev, device_id_type=MESH)

    loads = [
        (spec_h, xs), (tw_h, tws), (own_h.at[f], cb), (nb_h, nb), (gb_h, gb), (gc_h, gc),
        (ws_h, ws), (cp_h, cp), (basis_h, basis), (w_h, wf),
    ]
    local = [pltpu.make_async_copy(s, d, lsem.at[i]) for i, (s, d) in enumerate(loads)]
    for c in local:
        c.start()

    twf[...] = jnp.zeros_like(twf)
    xp[KP - 8 :, :] = jnp.zeros((8, NP), F32)
    sb[ROWS:, :] = jnp.zeros((EXT - ROWS, 256), BF16)
    local[0].wait()
    xp[0:FL, :] = xs[0]
    xp[FL : 2 * FL, :] = xs[1]
    local[1].wait()
    local[6].wait()
    hs[0] = ws[pl.ds(1, HALO, stride=2), :]
    hs[1] = ws[pl.ds(2 * (ROWS - HALO) + 1, HALO, stride=2), :]

    pl.semaphore_wait(bar, len(first))

    tw_c = [remote(tws, twr.at[f], tw_s.at[d], tw_r.at[d], fdev(d)) for d in range(1, FD)]
    for c in tw_c:
        c.start()

    def x_copy(h, d):
        to = lax.rem(f + d, FD)
        cols = pl.ds(pl.multiple_of(to * COLS + h * HC, 128), HC)
        rows = pl.ds(pl.multiple_of(f * KP, 8), KP)
        return remote(xp.at[:, cols], r.at[h, rows], x_s.at[h, d], x_r.at[h, d], (to, m))

    x_c = [[x_copy(h, d) for d in range(1, FD)] for h in range(HALVES)]
    for c in x_c[0]:
        c.start()
    for dev in xline:
        pl.semaphore_signal(mesh_sem, inc=1, device_id=dev, device_id_type=MESH)
    own_x = [
        pltpu.make_async_copy(
            xp.at[:, pl.ds(pl.multiple_of(f * COLS + h * HC, 128), HC)],
            r.at[h, pl.ds(pl.multiple_of(f * KP, 8), KP)],
            lsem.at[10 + h],
        )
        for h in range(HALVES)
    ]
    for c in own_x:
        c.start()

    local[2].wait()
    for c in tw_c:
        c.wait_recv()
    twr[f] = tws[...]
    for w in range(FD):
        twf[2 * w : 2 * w + 2, 0:TL] = twr[w]
    th, tl = split_bf16(twf[:, 0:64])
    g_all = dot(th, cb[0]) + dot(tl, cb[0]) + dot(th, cb[1])
    row_w = lax.broadcasted_iota(jnp.int32, (16, 128), 0) // 2
    lane_w = lax.broadcasted_iota(jnp.int32, (16, 128), 1) // 64
    g2 = jnp.zeros((16, 128), F32)
    for i in range(4):
        g2 = g2 + jnp.where(lane_w + 2 * i == row_w, g_all[:, 128 * i : 128 * (i + 1)], 0.0)
    g = (g2 + pltpu.roll(g2, 64, 1))[:, 0:KP]
    gh, gl = split_bf16(g)
    ghl = jnp.concatenate([gh, gl], axis=0)
    for q in range(8):
        xh, xl = split_bf16(xp[:, 512 * q : 512 * (q + 1)])
        both = dot(ghl, xh)
        part = both[0:16] + both[16:32] + dot(gh, xl)
        for b in range(4):
            pb[pl.ds(4 * q + b, 16, stride=NBLK), :] = part[:, 128 * b : 128 * (b + 1)]

    def a_copy(d):
        to = lax.rem(f + d, FD)
        return remote(pb.at[pl.ds(pl.multiple_of(to * 64, 8), 64)], ra.at[f], a_s.at[d], a_r.at[d], (to, m))

    a_c = [a_copy(d) for d in range(1, FD)]
    for c in a_c:
        c.start()
    for c in x_c[1]:
        c.start()
    ra[f] = pb[pl.ds(pl.multiple_of(f * 64, 8), 64), :]

    pl.semaphore_wait(mesh_sem, 3)
    up, down = mdev(1), mdev(MD - 1)

    def halo_pair(i, low_src, high_src, dst):
        return [
            remote(low_src, dst.at[1], h_s.at[i], h_r.at[i], down),
            remote(high_src, dst.at[0], h_s.at[i + 1], h_r.at[i + 1], up),
        ]

    cur_c = halo_pair(0, hs.at[0], hs.at[1], hcur)
    for c in cur_c:
        c.start()

    local[3].wait()
    nbv = nb[...]
    nbv = jnp.where(nbv >= ROWS + HALO, nbv, jnp.where(nbv < HALO, nbv + ROWS, nbv - HALO)).astype(F32)
    lane = lax.broadcasted_iota(jnp.int32, (128, 128), 1).astype(F32)
    for n in range(4):
        for ut in range(4):
            col = jnp.transpose(jnp.broadcast_to(nbv[n : n + 1, 128 * ut : 128 * (ut + 1)], (128, 128)))
            for kt in range(EXT // 128):
                hot = jnp.where(col == lane + float(128 * kt), 1.0, 0.0).astype(BF16)
                oh[ut, 128 * n : 128 * (n + 1), 128 * kt : 128 * (kt + 1)] = hot

    local[9].wait()

    def split_w(i, carry):
        rows = pl.ds(pl.multiple_of(i * 512, 512), 512)
        hi, lo = split_bf16(wf[rows, :])
        whl[rows, 0:128] = hi
        whl[rows, 128:256] = lo
        return carry

    lax.fori_loop(0, GROUPS * BLK // 512, split_w, 0)

    for i in (7,):
        local[i].wait()

    def put_ext(lo_row, value):
        hi, lo = split_bf16(value)
        sb[lo_row : lo_row + value.shape[0], 0:128] = hi
        sb[lo_row : lo_row + value.shape[0], 128:256] = lo

    def put_halo(buf):
        put_ext(ROWS, jnp.where(m > 0, buf[0], 0.0))
        put_ext(ROWS + HALO, jnp.where(m < MD - 1, buf[1], 0.0))

    def spread(ut, v):
        e = dot(oh[ut], sb[...])
        total = jnp.zeros((128, 128), F32)
        for n in range(4):
            c = cp[pl.ds(512 * ut + n, 128, stride=4), :]
            total = total + c * (e[128 * n : 128 * (n + 1), 0:128] + e[128 * n : 128 * (n + 1), 128:256] - v)
        return total

    put_ext(0, ws[pl.ds(1, ROWS, stride=2), :])
    for c in cur_c:
        c.wait_recv()
    put_halo(hcur)
    for ut in range(4):
        cur = ws[pl.ds(256 * ut + 1, 128, stride=2), :]
        prev = ws[pl.ds(256 * ut, 128, stride=2), :]
        base1[128 * ut : 128 * (ut + 1), :] = 2.0 * cur - prev + spread(ut, cur)
    b1_c = halo_pair(2, base1.at[0:HALO], base1.at[ROWS - HALO : ROWS], hb1)
    for c in b1_c:
        c.start()

    local[8].wait()

    def y_copy(h, d):
        to = lax.rem(f + d, FD)
        cols = pl.ds(pl.multiple_of(f * COLS + h * HC, 128), HC)
        return remote(s2.at[h, to], series_o.at[:, cols], y_s.at[h, d], y_r.at[h, d], (to, m))

    y_c = [[y_copy(h, d) for d in range(1, FD)] for h in range(HALVES)]
    own_y = []

    def transform(h):
        for c in x_c[h]:
            c.wait_recv()
        own_x[h].wait()
        xh, xl = split_bf16(r[h])
        out = dot(basis[0], xh) + dot(basis[0], xl) + dot(basis[1], xh)
        for w in range(FD):
            s2[h, w] = out[KP * w : KP * w + TL]
        for c in y_c[h]:
            c.start()
        c = pltpu.make_async_copy(
            s2.at[h, f], series_o.at[:, pl.ds(pl.multiple_of(f * COLS + h * HC, 128), HC)], lsem.at[12 + h]
        )
        c.start()
        own_y.append(c)

    transform(0)

    for c in a_c:
        c.wait_recv()
    total = ra[0]
    for i in range(1, FD):
        total = total + ra[i]
    wsum[...] = total
    ag[m] = total
    g_c = [remote(wsum, ag.at[m], g_s.at[d], g_r.at[d], mdev(d)) for d in range(1, MD)]
    for c in g_c:
        c.start()

    put_ext(0, base1[...])
    for c in b1_c:
        c.wait_recv()
    put_halo(hb1)
    for ut in range(4):
        cur = ws[pl.ds(256 * ut + 1, 128, stride=2), :]
        b1 = base1[128 * ut : 128 * (ut + 1), :]
        base2[128 * ut : 128 * (ut + 1), :] = 2.0 * b1 - cur + spread(ut, b1)

    transform(1)

    local[4].wait()
    local[5].wait()
    gbv = gb[...].astype(F32)
    index = lax.broadcasted_iota(jnp.int32, (1, 128), 1)
    gbv = jnp.where(index < gc[...], gbv, -1.0)
    gcol = jnp.transpose(jnp.broadcast_to(gbv, (128, 128)))
    pick = jnp.concatenate(
        [jnp.where(gcol == lane + float(128 * kt), 1.0, 0.0).astype(BF16) for kt in range(4)], axis=1
    )
    for c in g_c:
        c.wait_recv()
    for s in range(2):
        blocks = ag[:, NBLK * s : NBLK * (s + 1), :].reshape(MD * NBLK, BLK)
        hi, lo = split_bf16(blocks)
        ph = dot(pick, hi)
        lh[0, pl.ds(2 * s, 128, stride=4), :] = ph
        lh[1, pl.ds(2 * s, 128, stride=4), :] = ph
        lh[0, pl.ds(2 * s + 1, 128, stride=4), :] = dot(pick, lo)
        lh[1, pl.ds(2 * s + 1, 128, stride=4), :] = jnp.zeros((128, 128), F32)
    upper = lax.broadcasted_iota(jnp.int32, (8, 128), 0) < 4

    def interp(i, carry):
        for j in range(4):
            rows = pl.ds(pl.multiple_of(i * 32 + 8 * j, 8), 8)
            w = whl[pl.ds(pl.multiple_of(i * 1024 + 256 * j, 256), 256), :]
            left = jnp.concatenate([lh[0, rows, :], lh[1, rows, :]], axis=1).astype(BF16)
            out = dot_t(left, w)
            ee[rows, :] = jnp.where(upper, out[:, 0:128], out[:, 128:256])
        return carry

    lax.fori_loop(0, GROUPS // 8, interp, 0)
    push0 = ee[pl.ds(0, 128, stride=4), :] + ee[pl.ds(1, 128, stride=4), :]
    push1 = ee[pl.ds(2, 128, stride=4), :] + ee[pl.ds(3, 128, stride=4), :]
    hps[...] = push0[0:HALO]
    p_c = remote(hps, hpush, h_s.at[4], h_r.at[4], down)
    p_c.start()

    sb[ROWS : ROWS + HALO, :] = jnp.zeros((HALO, 256), BF16)
    put_ext(0, push0)
    p_c.wait_recv()
    put_ext(ROWS + HALO, jnp.where(m < MD - 1, hpush[...], 0.0))
    for ut in range(4):
        e = dot(oh[ut, :, 0:128], sb[0:128, :]) + dot(oh[ut, :, ROWS:EXT], sb[ROWS:EXT, :])
        total = jnp.zeros((128, 128), F32)
        for n in range(4):
            c = cp[pl.ds(512 * ut + n, 128, stride=4), :]
            en = e[128 * n : 128 * (n + 1), 0:128] + e[128 * n : 128 * (n + 1), 128:256]
            total = total + c * (en - push0 if ut == 0 else en)
        n1 = base1[128 * ut : 128 * (ut + 1), :]
        n2 = base2[128 * ut : 128 * (ut + 1), :] + total
        if ut == 0:
            n1 = n1 + push0
            n2 = n2 + 2.0 * push0 + push1
        ns[pl.ds(256 * ut, 128, stride=2), :] = n1
        ns[pl.ds(256 * ut + 1, 128, stride=2), :] = n2
    out_c = pltpu.make_async_copy(ns, state_o, lsem.at[14])
    out_c.start()

    for c in tw_c + x_c[0] + x_c[1] + a_c + g_c + cur_c + b1_c + [p_c] + y_c[0] + y_c[1]:
        c.wait_send()
    for c in y_c[0] + y_c[1]:
        c.wait_recv()
    for c in own_y:
        c.wait()
    out_c.wait()


def local_step(spectrum, time_weights, interp_weights, group_block, group_count, wave_state, neighbors, coupling):
    basis, own = host_basis()
    ws = wave_state.reshape(2, ROWS, 128).transpose(1, 0, 2).reshape(2 * ROWS, 128)
    cp = coupling.reshape(4, ROWS, 128).transpose(1, 0, 2).reshape(4 * ROWS, 128)
    any_spec = pl.BlockSpec(memory_space=pl.ANY)
    sem = pltpu.SemaphoreType.DMA
    series, state = pl.pallas_call(
        kernel,
        out_shape=(
            jax.ShapeDtypeStruct((TL, NP), F32),
            jax.ShapeDtypeStruct((2 * ROWS, 128), F32),
        ),
        in_specs=[any_spec] * 10,
        out_specs=(any_spec, any_spec),
        scratch_shapes=[
            pltpu.VMEM((2, FL, NP), F32),
            pltpu.VMEM((KP, NP), F32),
            pltpu.VMEM((2, TL), F32),
            pltpu.VMEM((FD, 2, TL), F32),
            pltpu.VMEM((16, 128), F32),
            pltpu.VMEM((2, 64, FD * 64), BF16),
            pltpu.VMEM((2, FD * KP, FD * KP), BF16),
            pltpu.VMEM((HALVES, FD * KP, HC), F32),
            pltpu.VMEM((HALVES, FD, TL, HC), F32),
            pltpu.VMEM((16 * NBLK, BLK), F32),
            pltpu.VMEM((FD, 64, BLK), F32),
            pltpu.VMEM((64, BLK), F32),
            pltpu.VMEM((MD, 64, BLK), F32),
            pltpu.VMEM((GROUPS * BLK, BLK), F32),
            pltpu.VMEM((GROUPS * BLK, 2 * BLK), BF16),
            pltpu.VMEM((4, 512, EXT), BF16),
            pltpu.VMEM((2 * ROWS, 128), F32),
            pltpu.VMEM((4 * ROWS, 128), F32),
            pltpu.VMEM((4, ROWS), jnp.int32),
            pltpu.VMEM((1, 128), jnp.int32),
            pltpu.VMEM((1, 1), jnp.int32),
            pltpu.VMEM((2, HALO, 128), F32),
            pltpu.VMEM((2, HALO, 128), F32),
            pltpu.VMEM((2, HALO, 128), F32),
            pltpu.VMEM((HALO, 128), F32),
            pltpu.VMEM((HALO, 128), F32),
            pltpu.VMEM((EXT, 256), BF16),
            pltpu.VMEM((ROWS, 128), F32),
            pltpu.VMEM((ROWS, 128), F32),
            pltpu.VMEM((2 * ROWS, 128), F32),
            pltpu.VMEM((2, 4 * GROUPS, BLK), F32),
            pltpu.VMEM((4 * GROUPS, BLK), F32),
            sem((16,)),
            sem((FD,)), sem((FD,)),
            sem((HALVES, FD)), sem((HALVES, FD)),
            sem((FD,)), sem((FD,)),
            sem((MD,)), sem((MD,)),
            sem((6,)), sem((6,)),
            sem((HALVES, FD)), sem((HALVES, FD)),
            pltpu.SemaphoreType.REGULAR,
        ],
        compiler_params=pltpu.CompilerParams(
            collective_id=0, has_side_effects=True, vmem_limit_bytes=58 * 1024 * 1024
        ),
        name="p2o_wave",
    )(
        spectrum, time_weights, interp_weights.reshape(GROUPS * BLK, BLK), group_block.reshape(1, GROUPS),
        group_count.reshape(1, 1), ws, neighbors, cp, jnp.asarray(basis), jnp.asarray(own),
    )
    new_state = state.reshape(ROWS, 2, 128).transpose(1, 0, 2).reshape(1, 2, ROWS * 128)
    return series, new_state


def solution(mesh):
    in_specs = (
        P(None, "freq", "mesh"),
        P(None, "freq"),
        P("mesh", None, None),
        P("mesh"),
        P("mesh"),
        P("freq", None, "mesh"),
        P(None, "mesh"),
        P(None, "mesh"),
    )
    out_specs = (P("freq", "mesh"), P("freq", None, "mesh"))
    return jax.shard_map(local_step, mesh=mesh, in_specs=in_specs, out_specs=out_specs, check_vma=False)
```

```python
import math

import jax
import jax.numpy as jnp
import numpy as np
from jax import lax
from jax.experimental import pallas as pl
from jax.experimental.pallas import tpu as pltpu
from jax.sharding import PartitionSpec as P

MESH = pl.DeviceIdType.MESH
F32 = jnp.float32
BF16 = jnp.bfloat16

NF = 216
NT = 432
FD = 8
MD = 16
FL = NF // FD
TL = NT // FD
KP = 56
NP = 4096
COLS = NP // FD
HALVES = 2
HC = COLS // HALVES
BLK = 128
NBLK = NP // BLK
GROUPS = 128
ROWS = 512
HALO = 32
EXT = 640


def split_bf16(x):
    hi = x.astype(BF16)
    lo = (x - hi.astype(F32)).astype(BF16)
    return hi, lo


def host_split(x):
    hi = np.asarray(x, np.float32).astype(jnp.bfloat16)
    lo = (x - hi.astype(np.float64)).astype(jnp.bfloat16)
    return hi, lo


def host_basis():
    t = np.arange(NT)[:, None]
    k = np.arange(NF)[None, :]
    angle = (t * k % NT) * (2.0 * math.pi / NT)
    scale = np.where(k == 0, 1.0, 2.0) / NT
    full = np.zeros((FD, KP, FD, KP))
    full[:, :TL, :, :FL] = (np.cos(angle) * scale).reshape(FD, TL, FD, FL)
    full[:, :TL, :, FL : 2 * FL] = (-np.sin(angle) * scale).reshape(FD, TL, FD, FL)
    basis = np.stack(host_split(full.reshape(FD * KP, FD * KP)))
    own = np.zeros((FD, 64, FD, 64))
    own[:, :KP, :, :KP] = full.transpose(2, 1, 0, 3)
    own = own.reshape(FD, 64, FD * 64)
    return basis, np.stack(host_split(own), axis=1)


def dot(a, b):
    return jnp.dot(a, b, preferred_element_type=F32)


def dot_t(a, b):
    return lax.dot_general(a, b, (((1,), (1,)), ((), ())), preferred_element_type=F32)


def kernel(
    spec_h, tw_h, w_h, gb_h, gc_h, ws_h, nb_h, cp_h, basis_h, own_h,
    series_o, state_o,
    xs, xp, tws, twr, twf, cb, basis, r, s2, pb, ra, wsum, ag, wf, whl, oh, ws, cp, nb, gb, gc,
    hs, hcur, hb1, hpush, hps, sb, base1, base2, lh, ee,
    lsem, tw_s, tw_r, x_s, x_r, a_s, a_r, g_s, g_r, h_s, h_r, y_s, y_r, mesh_sem,
):
    f = lax.axis_index("freq")
    m = lax.axis_index("mesh")
    z, x = m // 4, m % 4

    def fdev(d):
        return (lax.rem(f + d, FD), m)

    def mdev(d):
        return (f, lax.rem(m + d, MD))

    def remote(src, dst, ssem, rsem, dev):
        return pltpu.make_async_remote_copy(
            src_ref=src, dst_ref=dst, send_sem=ssem, recv_sem=rsem, device_id=dev, device_id_type=MESH
        )

    bar = pltpu.get_barrier_semaphore()
    xline = [(f, z * 4 + lax.rem(x + d, 4)) for d in range(1, 4)]
    zline = [(f, lax.rem(z + d, 4) * 4 + x) for d in range(1, 4)]
    first = [fdev(d) for d in range(1, FD)] + xline + zline
    for dev in first:
        pl.semaphore_signal(bar, inc=1, device_id=dev, device_id_type=MESH)

    loads = [
        (spec_h, xs), (tw_h, tws), (own_h.at[f], cb), (nb_h, nb), (gb_h, gb), (gc_h, gc),
        (ws_h, ws), (cp_h, cp), (basis_h, basis), (w_h, wf),
    ]
    local = [pltpu.make_async_copy(s, d, lsem.at[i]) for i, (s, d) in enumerate(loads)]
    for c in local:
        c.start()

    twf[...] = jnp.zeros_like(twf)
    xp[KP - 8 :, :] = jnp.zeros((8, NP), F32)
    sb[ROWS:, :] = jnp.zeros((EXT - ROWS, 256), BF16)
    local[0].wait()
    for ct in range(NBLK):
        for part in range(2):
            xp[FL * part : FL * (part + 1), BLK * ct : BLK * (ct + 1)] = xs[pl.ds(2 * ct + part, FL, stride=2 * NBLK), :]
    local[1].wait()
    local[6].wait()
    hs[0] = ws[pl.ds(1, HALO, stride=2), :]
    hs[1] = ws[pl.ds(2 * (ROWS - HALO) + 1, HALO, stride=2), :]

    pl.semaphore_wait(bar, len(first))

    tw_c = [remote(tws, twr.at[f], tw_s.at[d], tw_r.at[d], fdev(d)) for d in range(1, FD)]
    for c in tw_c:
        c.start()

    def x_copy(h, d):
        to = lax.rem(f + d, FD)
        cols = pl.ds(pl.multiple_of(to * COLS + h * HC, 128), HC)
        rows = pl.ds(pl.multiple_of(f * KP, 8), KP)
        return remote(xp.at[:, cols], r.at[h, rows], x_s.at[h, d], x_r.at[h, d], (to, m))

    x_c = [[x_copy(h, d) for d in range(1, FD)] for h in range(HALVES)]
    for c in x_c[0]:
        c.start()
    for dev in xline:
        pl.semaphore_signal(mesh_sem, inc=1, device_id=dev, device_id_type=MESH)
    own_x = [
        pltpu.make_async_copy(
            xp.at[:, pl.ds(pl.multiple_of(f * COLS + h * HC, 128), HC)],
            r.at[h, pl.ds(pl.multiple_of(f * KP, 8), KP)],
            lsem.at[10 + h],
        )
        for h in range(HALVES)
    ]
    for c in own_x:
        c.start()

    local[2].wait()
    for c in tw_c:
        c.wait_recv()
    twr[f] = tws[...]
    for w in range(FD):
        twf[2 * w : 2 * w + 2, 0:TL] = twr[w]
    th, tl = split_bf16(twf[:, 0:64])
    g_all = dot(th, cb[0]) + dot(tl, cb[0]) + dot(th, cb[1])
    row_w = lax.broadcasted_iota(jnp.int32, (16, 128), 0) // 2
    lane_w = lax.broadcasted_iota(jnp.int32, (16, 128), 1) // 64
    g2 = jnp.zeros((16, 128), F32)
    for i in range(4):
        g2 = g2 + jnp.where(lane_w + 2 * i == row_w, g_all[:, 128 * i : 128 * (i + 1)], 0.0)
    g = (g2 + pltpu.roll(g2, 64, 1))[:, 0:KP]
    gh, gl = split_bf16(g)
    ghl = jnp.concatenate([gh, gl], axis=0)
    for q in range(8):
        xh, xl = split_bf16(xp[:, 512 * q : 512 * (q + 1)])
        both = dot(ghl, xh)
        part = both[0:16] + both[16:32] + dot(gh, xl)
        for b in range(4):
            pb[pl.ds(4 * q + b, 16, stride=NBLK), :] = part[:, 128 * b : 128 * (b + 1)]

    def a_copy(d):
        to = lax.rem(f + d, FD)
        return remote(pb.at[pl.ds(pl.multiple_of(to * 64, 8), 64)], ra.at[f], a_s.at[d], a_r.at[d], (to, m))

    a_c = [a_copy(d) for d in range(1, FD)]
    for c in a_c:
        c.start()
    for c in x_c[1]:
        c.start()
    ra[f] = pb[pl.ds(pl.multiple_of(f * 64, 8), 64), :]

    pl.semaphore_wait(mesh_sem, 3)
    up, down = mdev(1), mdev(MD - 1)

    def halo_pair(i, low_src, high_src, dst):
        return [
            remote(low_src, dst.at[1], h_s.at[i], h_r.at[i], down),
            remote(high_src, dst.at[0], h_s.at[i + 1], h_r.at[i + 1], up),
        ]

    cur_c = halo_pair(0, hs.at[0], hs.at[1], hcur)
    for c in cur_c:
        c.start()

    local[3].wait()
    nbv = nb[...]
    nbv = jnp.where(nbv >= ROWS + HALO, nbv, jnp.where(nbv < HALO, nbv + ROWS, nbv - HALO)).astype(F32)
    lane = lax.broadcasted_iota(jnp.int32, (128, 128), 1).astype(F32)
    for n in range(4):
        for ut in range(4):
            col = jnp.transpose(jnp.broadcast_to(nbv[n : n + 1, 128 * ut : 128 * (ut + 1)], (128, 128)))
            for kt in range(EXT // 128):
                hot = jnp.where(col == lane + float(128 * kt), 1.0, 0.0).astype(BF16)
                oh[ut, 128 * n : 128 * (n + 1), 128 * kt : 128 * (kt + 1)] = hot

    local[9].wait()

    def split_w(i, carry):
        rows = pl.ds(pl.multiple_of(i * 512, 512), 512)
        hi, lo = split_bf16(wf[rows, :])
        whl[rows, 0:128] = hi
        whl[rows, 128:256] = lo
        return carry

    lax.fori_loop(0, GROUPS * BLK // 512, split_w, 0)

    for i in (7,):
        local[i].wait()

    def put_ext(lo_row, value):
        hi, lo = split_bf16(value)
        sb[lo_row : lo_row + value.shape[0], 0:128] = hi
        sb[lo_row : lo_row + value.shape[0], 128:256] = lo

    def put_halo(buf):
        put_ext(ROWS, jnp.where(m > 0, buf[0], 0.0))
        put_ext(ROWS + HALO, jnp.where(m < MD - 1, buf[1], 0.0))

    def spread(ut, v):
        e = dot(oh[ut], sb[...])
        total = jnp.zeros((128, 128), F32)
        for n in range(4):
            c = cp[pl.ds(512 * ut + n, 128, stride=4), :]
            total = total + c * (e[128 * n : 128 * (n + 1), 0:128] + e[128 * n : 128 * (n + 1), 128:256] - v)
        return total

    put_ext(0, ws[pl.ds(1, ROWS, stride=2), :])
    for c in cur_c:
        c.wait_recv()
    put_halo(hcur)
    for ut in range(4):
        cur = ws[pl.ds(256 * ut + 1, 128, stride=2), :]
        prev = ws[pl.ds(256 * ut, 128, stride=2), :]
        base1[128 * ut : 128 * (ut + 1), :] = 2.0 * cur - prev + spread(ut, cur)
    b1_c = halo_pair(2, base1.at[0:HALO], base1.at[ROWS - HALO : ROWS], hb1)
    for c in b1_c:
        c.start()

    local[8].wait()

    def y_copy(h, d):
        to = lax.rem(f + d, FD)
        cols = pl.ds(pl.multiple_of(f * COLS + h * HC, 128), HC)
        return remote(s2.at[h, to], series_o.at[:, cols], y_s.at[h, d], y_r.at[h, d], (to, m))

    y_c = [[y_copy(h, d) for d in range(1, FD)] for h in range(HALVES)]
    own_y = []

    def transform(h):
        for c in x_c[h]:
            c.wait_recv()
        own_x[h].wait()
        xh, xl = split_bf16(r[h])
        out = dot(basis[0], xh) + dot(basis[0], xl) + dot(basis[1], xh)
        for w in range(FD):
            s2[h, w] = out[KP * w : KP * w + TL]
        for c in y_c[h]:
            c.start()
        c = pltpu.make_async_copy(
            s2.at[h, f], series_o.at[:, pl.ds(pl.multiple_of(f * COLS + h * HC, 128), HC)], lsem.at[12 + h]
        )
        c.start()
        own_y.append(c)

    transform(0)

    for c in a_c:
        c.wait_recv()
    total = ra[0]
    for i in range(1, FD):
        total = total + ra[i]
    wsum[...] = total
    ag[m] = total
    g_c = [remote(wsum, ag.at[m], g_s.at[d], g_r.at[d], mdev(d)) for d in range(1, MD)]
    for c in g_c:
        c.start()

    put_ext(0, base1[...])
    for c in b1_c:
        c.wait_recv()
    put_halo(hb1)
    for ut in range(4):
        cur = ws[pl.ds(256 * ut + 1, 128, stride=2), :]
        b1 = base1[128 * ut : 128 * (ut + 1), :]
        base2[128 * ut : 128 * (ut + 1), :] = 2.0 * b1 - cur + spread(ut, b1)

    transform(1)

    local[4].wait()
    local[5].wait()
    gbv = gb[...].astype(F32)
    index = lax.broadcasted_iota(jnp.int32, (1, 128), 1)
    gbv = jnp.where(index < gc[...], gbv, -1.0)
    gcol = jnp.transpose(jnp.broadcast_to(gbv, (128, 128)))
    pick = jnp.concatenate(
        [jnp.where(gcol == lane + float(128 * kt), 1.0, 0.0).astype(BF16) for kt in range(4)], axis=1
    )
    for c in g_c:
        c.wait_recv()
    for s in range(2):
        blocks = ag[:, NBLK * s : NBLK * (s + 1), :].reshape(MD * NBLK, BLK)
        hi, lo = split_bf16(blocks)
        ph = dot(pick, hi)
        lh[0, pl.ds(2 * s, 128, stride=4), :] = ph
        lh[1, pl.ds(2 * s, 128, stride=4), :] = ph
        lh[0, pl.ds(2 * s + 1, 128, stride=4), :] = dot(pick, lo)
        lh[1, pl.ds(2 * s + 1, 128, stride=4), :] = jnp.zeros((128, 128), F32)
    upper = lax.broadcasted_iota(jnp.int32, (8, 128), 0) < 4

    def interp(i, carry):
        for j in range(4):
            rows = pl.ds(pl.multiple_of(i * 32 + 8 * j, 8), 8)
            w = whl[pl.ds(pl.multiple_of(i * 1024 + 256 * j, 256), 256), :]
            left = jnp.concatenate([lh[0, rows, :], lh[1, rows, :]], axis=1).astype(BF16)
            out = dot_t(left, w)
            ee[rows, :] = jnp.where(upper, out[:, 0:128], out[:, 128:256])
        return carry

    lax.fori_loop(0, GROUPS // 8, interp, 0)
    push0 = ee[pl.ds(0, 128, stride=4), :] + ee[pl.ds(1, 128, stride=4), :]
    push1 = ee[pl.ds(2, 128, stride=4), :] + ee[pl.ds(3, 128, stride=4), :]
    hps[...] = push0[0:HALO]
    p_c = remote(hps, hpush, h_s.at[4], h_r.at[4], down)
    p_c.start()

    sb[ROWS : ROWS + HALO, :] = jnp.zeros((HALO, 256), BF16)
    put_ext(0, push0)
    p_c.wait_recv()
    put_ext(ROWS + HALO, jnp.where(m < MD - 1, hpush[...], 0.0))
    for ut in range(4):
        e = dot(oh[ut, :, 0:128], sb[0:128, :]) + dot(oh[ut, :, ROWS:EXT], sb[ROWS:EXT, :])
        total = jnp.zeros((128, 128), F32)
        for n in range(4):
            c = cp[pl.ds(512 * ut + n, 128, stride=4), :]
            en = e[128 * n : 128 * (n + 1), 0:128] + e[128 * n : 128 * (n + 1), 128:256]
            total = total + c * (en - push0 if ut == 0 else en)
        n1 = base1[128 * ut : 128 * (ut + 1), :]
        n2 = base2[128 * ut : 128 * (ut + 1), :] + total
        if ut == 0:
            n1 = n1 + push0
            n2 = n2 + 2.0 * push0 + push1
        state_o[pl.ds(256 * ut, 128, stride=2), :] = n1
        state_o[pl.ds(256 * ut + 1, 128, stride=2), :] = n2

    for c in tw_c + x_c[0] + x_c[1] + a_c + g_c + cur_c + b1_c + [p_c] + y_c[0] + y_c[1]:
        c.wait_send()
    for c in y_c[0] + y_c[1]:
        c.wait_recv()
    for c in own_y:
        c.wait()


def local_step(spectrum, time_weights, interp_weights, group_block, group_count, wave_state, neighbors, coupling):
    basis, own = host_basis()
    ws = wave_state.reshape(2, ROWS, 128).transpose(1, 0, 2).reshape(2 * ROWS, 128)
    cp = coupling.reshape(4, ROWS, 128).transpose(1, 0, 2).reshape(4 * ROWS, 128)
    hbm_spec = pl.BlockSpec(memory_space=pltpu.HBM)
    vmem_spec = pl.BlockSpec(memory_space=pltpu.VMEM)
    sem = pltpu.SemaphoreType.DMA
    spec = spectrum.reshape(2, FL, NBLK, BLK).transpose(1, 2, 0, 3).reshape(FL * 2 * NBLK, BLK)
    series, state = pl.pallas_call(
        kernel,
        out_shape=(pltpu.VMEM((TL, NP), F32), pltpu.VMEM((2 * ROWS, 128), F32)),
        in_specs=[hbm_spec] * 10,
        out_specs=(vmem_spec, vmem_spec),
        scratch_shapes=[
            pltpu.VMEM((FL * 2 * NBLK, BLK), F32),
            pltpu.VMEM((KP, NP), F32),
            pltpu.VMEM((2, TL), F32),
            pltpu.VMEM((FD, 2, TL), F32),
            pltpu.VMEM((16, 128), F32),
            pltpu.VMEM((2, 64, FD * 64), BF16),
            pltpu.VMEM((2, FD * KP, FD * KP), BF16),
            pltpu.VMEM((HALVES, FD * KP, HC), F32),
            pltpu.VMEM((HALVES, FD, TL, HC), F32),
            pltpu.VMEM((16 * NBLK, BLK), F32),
            pltpu.VMEM((FD, 64, BLK), F32),
            pltpu.VMEM((64, BLK), F32),
            pltpu.VMEM((MD, 64, BLK), F32),
            pltpu.VMEM((GROUPS * BLK, BLK), F32),
            pltpu.VMEM((GROUPS * BLK, 2 * BLK), BF16),
            pltpu.VMEM((4, 512, EXT), BF16),
            pltpu.VMEM((2 * ROWS, 128), F32),
            pltpu.VMEM((4 * ROWS, 128), F32),
            pltpu.VMEM((4, ROWS), jnp.int32),
            pltpu.VMEM((1, 128), jnp.int32),
            pltpu.VMEM((1, 1), jnp.int32),
            pltpu.VMEM((2, HALO, 128), F32),
            pltpu.VMEM((2, HALO, 128), F32),
            pltpu.VMEM((2, HALO, 128), F32),
            pltpu.VMEM((HALO, 128), F32),
            pltpu.VMEM((HALO, 128), F32),
            pltpu.VMEM((EXT, 256), BF16),
            pltpu.VMEM((ROWS, 128), F32),
            pltpu.VMEM((ROWS, 128), F32),
            pltpu.VMEM((2, 4 * GROUPS, BLK), F32),
            pltpu.VMEM((4 * GROUPS, BLK), F32),
            sem((16,)),
            sem((FD,)), sem((FD,)),
            sem((HALVES, FD)), sem((HALVES, FD)),
            sem((FD,)), sem((FD,)),
            sem((MD,)), sem((MD,)),
            sem((6,)), sem((6,)),
            sem((HALVES, FD)), sem((HALVES, FD)),
            pltpu.SemaphoreType.REGULAR,
        ],
        compiler_params=pltpu.CompilerParams(
            collective_id=0, has_side_effects=True, vmem_limit_bytes=62 * 1024 * 1024
        ),
        name="p2o_wave",
    )(
        spec, time_weights, interp_weights.reshape(GROUPS * BLK, BLK), group_block.reshape(1, GROUPS),
        group_count.reshape(1, 1), ws, neighbors, cp, jnp.asarray(basis), jnp.asarray(own),
    )
    new_state = state.reshape(ROWS, 2, 128).transpose(1, 0, 2).reshape(1, 2, ROWS * 128)
    return series, new_state


def solution(mesh):
    in_specs = (
        P(None, "freq", "mesh"),
        P(None, "freq"),
        P("mesh", None, None),
        P("mesh"),
        P("mesh"),
        P("freq", None, "mesh"),
        P(None, "mesh"),
        P(None, "mesh"),
    )
    out_specs = (P("freq", "mesh"), P("freq", None, "mesh"))
    return jax.shard_map(local_step, mesh=mesh, in_specs=in_specs, out_specs=out_specs, check_vma=False)
```

```python
import functools
import math

import jax
import jax.numpy as jnp
import numpy as np
from jax import lax
from jax.experimental import pallas as pl
from jax.experimental.pallas import tpu as pltpu
from jax.sharding import PartitionSpec as P

MESH = pl.DeviceIdType.MESH
F32 = jnp.float32
BF16 = jnp.bfloat16

NF = 216
NT = 432
FD = 8
MD = 16
FL = NF // FD
TL = NT // FD
KP = 56
NP = 4096
COLS = NP // FD
HALVES = 2
HC = COLS // HALVES
BLK = 128
NBLK = NP // BLK
GROUPS = 128
ROWS = 512
HALO = 32
EXT = 640
SLOTS = 8


def split_bf16(x):
    hi = x.astype(BF16)
    lo = (x - hi.astype(F32)).astype(BF16)
    return hi, lo


def host_split(x):
    hi = np.asarray(x, np.float32).astype(jnp.bfloat16)
    lo = (x - hi.astype(np.float64)).astype(jnp.bfloat16)
    return hi, lo


def host_basis():
    t = np.arange(NT)[:, None]
    k = np.arange(NF)[None, :]
    angle = (t * k % NT) * (2.0 * math.pi / NT)
    scale = np.where(k == 0, 1.0, 2.0) / NT
    full = np.zeros((FD, KP, FD, KP))
    full[:, :TL, :, :FL] = (np.cos(angle) * scale).reshape(FD, TL, FD, FL)
    full[:, :TL, :, FL : 2 * FL] = (-np.sin(angle) * scale).reshape(FD, TL, FD, FL)
    basis = np.stack(host_split(full.reshape(FD * KP, FD * KP)))
    own = np.zeros((FD, 64, FD, 64))
    own[:, :KP, :, :KP] = full.transpose(2, 1, 0, 3)
    own = own.reshape(FD, 64, FD * 64)
    return basis, np.stack(host_split(own), axis=1)


def dot(a, b):
    return jnp.dot(a, b, preferred_element_type=F32)


def dot_t(a, b):
    return lax.dot_general(a, b, (((1,), (1,)), ((), ())), preferred_element_type=F32)


def kernel(
    spec_h, tw_h, w_h, gb_h, gc_h, ws_h, nb_h, cp_h, basis_h, own_h,
    series_o, state_o,
    xs, xp, tws, twr, twf, cb, basis, r, s2, pb, ra, rs, rq, pt, gs, gr, wf, whl, oh, ws, cp, nb, gb, gc,
    hs, hcur, hb1, hpush, hps, sb, base1, base2, lh, ee,
    lsem, tw_s, tw_r, x_s, x_r, a_s, a_r, q_s, q_r, g_s, g_r, h_s, h_r, y_s, y_r, mesh_sem,
):
    f = lax.axis_index("freq")
    m = lax.axis_index("mesh")

    def fdev(d):
        return (lax.rem(f + d, FD), m)

    def mdev(d):
        return (f, lax.rem(m + d, MD))

    def remote(src, dst, ssem, rsem, dev):
        return pltpu.make_async_remote_copy(
            src_ref=src, dst_ref=dst, send_sem=ssem, recv_sem=rsem, device_id=dev, device_id_type=MESH
        )

    bar = pltpu.get_barrier_semaphore()

    def tell(sem, dev):
        pl.semaphore_signal(sem, inc=1, device_id=dev, device_id_type=MESH)

    for d in range(1, FD):
        tell(bar, fdev(d))
    for d in range(1, MD):
        pl.when(m + d < MD)(functools.partial(tell, bar, mdev(d)))

    loads = [
        (spec_h, xs), (tw_h, tws), (own_h.at[f], cb), (nb_h, nb), (gb_h, gb), (gc_h, gc),
        (ws_h, ws), (cp_h, cp), (basis_h, basis), (w_h, wf),
    ]
    local = [pltpu.make_async_copy(s, d, lsem.at[i]) for i, (s, d) in enumerate(loads)]
    for c in local[:7]:
        c.start()

    twf[...] = jnp.zeros_like(twf)
    xp[KP - 8 :, :] = jnp.zeros((8, NP), F32)
    sb[ROWS:, :] = jnp.zeros((EXT - ROWS, 256), BF16)
    local[0].wait()
    for ct in range(NBLK):
        for part in range(2):
            xp[FL * part : FL * (part + 1), BLK * ct : BLK * (ct + 1)] = xs[pl.ds(2 * ct + part, FL, stride=2 * NBLK), :]
    local[1].wait()
    local[6].wait()
    hs[0] = ws[pl.ds(1, HALO, stride=2), :]
    hs[1] = ws[pl.ds(2 * (ROWS - HALO) + 1, HALO, stride=2), :]

    pl.semaphore_wait(bar, FD - 1 + m)

    tw_c = [remote(tws, twr.at[f], tw_s.at[d], tw_r.at[d], fdev(d)) for d in range(1, FD)]
    for c in tw_c:
        c.start()

    def x_copy(h, d):
        to = lax.rem(f + d, FD)
        cols = pl.ds(pl.multiple_of(to * COLS + h * HC, 128), HC)
        rows = pl.ds(pl.multiple_of(f * KP, 8), KP)
        return remote(xp.at[:, cols], r.at[h, rows], x_s.at[h, d], x_r.at[h, d], (to, m))

    x_c = [[x_copy(h, d) for d in range(1, FD)] for h in range(HALVES)]
    for c in x_c[0]:
        c.start()
    for d in range(1, MD):
        pl.when(m >= d)(functools.partial(tell, mesh_sem, mdev(MD - d)))
    for c in local[7:]:
        c.start()
    own_x = [
        pltpu.make_async_copy(
            xp.at[:, pl.ds(pl.multiple_of(f * COLS + h * HC, 128), HC)],
            r.at[h, pl.ds(pl.multiple_of(f * KP, 8), KP)],
            lsem.at[10 + h],
        )
        for h in range(HALVES)
    ]
    for c in own_x:
        c.start()

    local[4].wait()
    local[5].wait()
    index = lax.broadcasted_iota(jnp.int32, (1, GROUPS), 1)
    live = index < gc[0]
    gbv = gb[...]
    owner = jnp.where(live, lax.shift_right_logical(gbv, 5), -1).astype(F32)
    inner = (lax.bitwise_and(gbv, NBLK - 1) + 1).astype(F32)
    lane_i = lax.broadcasted_iota(jnp.int32, (128, 128), 1)
    lane = lane_i.astype(F32)
    owner_r = jnp.broadcast_to(owner, (128, 128))
    owner_c = jnp.transpose(owner_r)
    earlier = lane_i < lax.broadcasted_iota(jnp.int32, (128, 128), 0)
    rank = jnp.sum(jnp.where(jnp.logical_and(owner_r == owner_c, earlier), 1.0, 0.0), axis=1, keepdims=True)
    slot = jnp.where(owner_c >= 0.0, owner_c * SLOTS + rank, -1.0)
    place = jnp.where(slot == lane, 1.0, 0.0)
    asked = jnp.sum(jnp.transpose(place) * inner, axis=1, keepdims=True) - 1.0
    rs[...] = jnp.broadcast_to(asked, (128, 128))
    pt[...] = place.astype(BF16)

    def q_copy(d):
        to = lax.rem(m + d, MD)
        src = rs.at[pl.ds(pl.multiple_of(to * SLOTS, 8), SLOTS)]
        dst = rq.at[pl.ds(pl.multiple_of(m * SLOTS, 8), SLOTS)]
        return remote(src, dst, q_s.at[d], q_r.at[d], (f, to))

    q_c = [q_copy(d) for d in range(1, MD)]
    rq[pl.ds(pl.multiple_of(m * SLOTS, 8), SLOTS), :] = rs[pl.ds(pl.multiple_of(m * SLOTS, 8), SLOTS), :]
    up, down = mdev(1), mdev(MD - 1)
    above, below = m < MD - 1, m > 0

    def halo_pair(i, low_src, high_src, dst):
        return [
            (remote(low_src, dst.at[1], h_s.at[i], h_r.at[i], down), below, above),
            (remote(high_src, dst.at[0], h_s.at[i + 1], h_r.at[i + 1], up), above, below),
        ]

    def start_all(pairs):
        for c, sends, _ in pairs:
            pl.when(sends)(functools.partial(c.start))

    def recv_all(pairs):
        for c, _, gets in pairs:
            pl.when(gets)(c.wait_recv)

    cur_c = halo_pair(0, hs.at[0], hs.at[1], hcur)

    def enter_mesh():
        pl.when(above)(lambda: pl.semaphore_wait(mesh_sem, MD - 1 - m))
        for c in q_c:
            c.start()
        start_all(cur_c)

    pl.when(m >= MD // 2)(enter_mesh)

    local[2].wait()
    for c in tw_c:
        c.wait_recv()
    twr[f] = tws[...]
    for w in range(FD):
        twf[2 * w : 2 * w + 2, 0:TL] = twr[w]
    th, tl = split_bf16(twf[:, 0:64])
    g_all = dot(th, cb[0]) + dot(tl, cb[0]) + dot(th, cb[1])
    row_w = lax.broadcasted_iota(jnp.int32, (16, 128), 0) // 2
    lane_w = lax.broadcasted_iota(jnp.int32, (16, 128), 1) // 64
    g2 = jnp.zeros((16, 128), F32)
    for i in range(4):
        g2 = g2 + jnp.where(lane_w + 2 * i == row_w, g_all[:, 128 * i : 128 * (i + 1)], 0.0)
    g = (g2 + pltpu.roll(g2, 64, 1))[:, 0:KP]
    gh, gl = split_bf16(g)
    ghl = jnp.concatenate([gh, gl], axis=0)
    for q in range(8):
        xh, xl = split_bf16(xp[:, 512 * q : 512 * (q + 1)])
        both = dot(ghl, xh)
        part = both[0:16] + both[16:32] + dot(gh, xl)
        for b in range(4):
            pb[pl.ds(4 * q + b, 16, stride=NBLK), :] = part[:, 128 * b : 128 * (b + 1)]

    def a_copy(d):
        to = lax.rem(f + d, FD)
        return remote(pb.at[pl.ds(pl.multiple_of(to * 64, 8), 64)], ra.at[f], a_s.at[d], a_r.at[d], (to, m))

    a_c = [a_copy(d) for d in range(1, FD)]
    for c in a_c:
        c.start()
    for c in x_c[1]:
        c.start()
    ra[f] = pb[pl.ds(pl.multiple_of(f * 64, 8), 64), :]

    local[3].wait()
    nbv = nb[...]
    nbv = jnp.where(nbv >= ROWS + HALO, nbv, jnp.where(nbv < HALO, nbv + ROWS, nbv - HALO)).astype(F32)
    for n in range(4):
        for ut in range(4):
            col = jnp.transpose(jnp.broadcast_to(nbv[n : n + 1, 128 * ut : 128 * (ut + 1)], (128, 128)))
            for kt in range(EXT // 128):
                hot = jnp.where(col == lane + float(128 * kt), 1.0, 0.0).astype(BF16)
                oh[ut, 128 * n : 128 * (n + 1), 128 * kt : 128 * (kt + 1)] = hot

    local[9].wait()

    def split_w(i, carry):
        rows = pl.ds(pl.multiple_of(i * 512, 512), 512)
        hi, lo = split_bf16(wf[rows, :])
        whl[rows, 0:128] = hi
        whl[rows, 128:256] = lo
        return carry

    lax.fori_loop(0, GROUPS * BLK // 512, split_w, 0)

    pl.when(m < MD // 2)(enter_mesh)

    local[8].wait()

    def y_copy(h, d):
        to = lax.rem(f + d, FD)
        cols = pl.ds(pl.multiple_of(f * COLS + h * HC, 128), HC)
        return remote(s2.at[h, to], series_o.at[:, cols], y_s.at[h, d], y_r.at[h, d], (to, m))

    y_c = [[y_copy(h, d) for d in range(1, FD)] for h in range(HALVES)]
    own_y = []

    def transform(h):
        for c in x_c[h]:
            c.wait_recv()
        own_x[h].wait()
        xh, xl = split_bf16(r[h])
        out = dot(basis[0], xh) + dot(basis[0], xl) + dot(basis[1], xh)
        for w in range(FD):
            s2[h, w] = out[KP * w : KP * w + TL]
        for c in y_c[h]:
            c.start()
        c = pltpu.make_async_copy(
            s2.at[h, f], series_o.at[:, pl.ds(pl.multiple_of(f * COLS + h * HC, 128), HC)], lsem.at[12 + h]
        )
        c.start()
        own_y.append(c)


    transform(0)

    for c in q_c:
        c.wait_recv()
    sel = jnp.where(rq[...] == lane, 1.0, 0.0).astype(BF16)[:, 0:NBLK]
    for c in a_c:
        c.wait_recv()
    total = ra[0]
    for i in range(1, FD):
        total = total + ra[i]
    hi, lo = split_bf16(total)
    for s in range(2):
        rows = slice(NBLK * s, NBLK * (s + 1))
        out = dot(sel, hi[rows]) + dot(sel, lo[rows])
        for o in range(MD):
            gs[o, SLOTS * s : SLOTS * (s + 1), :] = out[SLOTS * o : SLOTS * (o + 1)]

    def g_copy(d):
        to = lax.rem(m + d, MD)
        return remote(gs.at[to], gr.at[m], g_s.at[d], g_r.at[d], (f, to))

    g_c = [g_copy(d) for d in range(1, MD)]
    for c in g_c:
        c.start()
    gr[m] = gs[m]

    transform(1)

    for i in (7,):
        local[i].wait()

    def put_ext(lo_row, value):
        hi, lo = split_bf16(value)
        sb[lo_row : lo_row + value.shape[0], 0:128] = hi
        sb[lo_row : lo_row + value.shape[0], 128:256] = lo

    def put_halo(buf):
        put_ext(ROWS, jnp.where(m > 0, buf[0], 0.0))
        put_ext(ROWS + HALO, jnp.where(m < MD - 1, buf[1], 0.0))

    def spread(ut, v):
        e = dot(oh[ut], sb[...])
        total = jnp.zeros((128, 128), F32)
        for n in range(4):
            c = cp[pl.ds(512 * ut + n, 128, stride=4), :]
            total = total + c * (e[128 * n : 128 * (n + 1), 0:128] + e[128 * n : 128 * (n + 1), 128:256] - v)
        return total

    put_ext(0, ws[pl.ds(1, ROWS, stride=2), :])
    recv_all(cur_c)
    put_halo(hcur)
    for ut in range(4):
        cur = ws[pl.ds(256 * ut + 1, 128, stride=2), :]
        prev = ws[pl.ds(256 * ut, 128, stride=2), :]
        base1[128 * ut : 128 * (ut + 1), :] = 2.0 * cur - prev + spread(ut, cur)
    b1_c = halo_pair(2, base1.at[0:HALO], base1.at[ROWS - HALO : ROWS], hb1)
    start_all(b1_c)

    for c in g_c:
        c.wait_recv()
    for s in range(2):
        blocks = gr[:, SLOTS * s : SLOTS * (s + 1), :].reshape(MD * SLOTS, BLK)
        hi, lo = split_bf16(blocks)
        ph = dot(pt[...], hi)
        lh[0, pl.ds(2 * s, 128, stride=4), :] = ph
        lh[1, pl.ds(2 * s, 128, stride=4), :] = ph
        lh[0, pl.ds(2 * s + 1, 128, stride=4), :] = dot(pt[...], lo)
        lh[1, pl.ds(2 * s + 1, 128, stride=4), :] = jnp.zeros((128, 128), F32)
    upper = lax.broadcasted_iota(jnp.int32, (8, 128), 0) < 4

    def interp(i, carry):
        for j in range(16):
            rows = pl.ds(pl.multiple_of(i * 128 + 8 * j, 8), 8)
            w = whl[pl.ds(pl.multiple_of(i * 4096 + 256 * j, 256), 256), :]
            left = jnp.concatenate([lh[0, rows, :], lh[1, rows, :]], axis=1).astype(BF16)
            out = dot_t(left, w)
            ee[rows, :] = jnp.where(upper, out[:, 0:128], out[:, 128:256])
        return carry

    lax.fori_loop(0, GROUPS // 32, interp, 0)
    push0 = ee[pl.ds(0, 128, stride=4), :] + ee[pl.ds(1, 128, stride=4), :]
    push1 = ee[pl.ds(2, 128, stride=4), :] + ee[pl.ds(3, 128, stride=4), :]
    hps[...] = push0[0:HALO]
    p_c = [(remote(hps, hpush, h_s.at[4], h_r.at[4], down), below, above)]
    start_all(p_c)

    put_ext(0, base1[...])
    recv_all(b1_c)
    put_halo(hb1)
    for ut in range(4):
        cur = ws[pl.ds(256 * ut + 1, 128, stride=2), :]
        b1 = base1[128 * ut : 128 * (ut + 1), :]
        base2[128 * ut : 128 * (ut + 1), :] = 2.0 * b1 - cur + spread(ut, b1)

    sb[ROWS : ROWS + HALO, :] = jnp.zeros((HALO, 256), BF16)
    put_ext(0, push0)
    recv_all(p_c)
    put_ext(ROWS + HALO, jnp.where(m < MD - 1, hpush[...], 0.0))
    for ut in range(4):
        e = dot(oh[ut, :, 0:128], sb[0:128, :]) + dot(oh[ut, :, ROWS:EXT], sb[ROWS:EXT, :])
        total = jnp.zeros((128, 128), F32)
        for n in range(4):
            c = cp[pl.ds(512 * ut + n, 128, stride=4), :]
            en = e[128 * n : 128 * (n + 1), 0:128] + e[128 * n : 128 * (n + 1), 128:256]
            total = total + c * (en - push0 if ut == 0 else en)
        n1 = base1[128 * ut : 128 * (ut + 1), :]
        n2 = base2[128 * ut : 128 * (ut + 1), :] + total
        if ut == 0:
            n1 = n1 + push0
            n2 = n2 + 2.0 * push0 + push1
        state_o[pl.ds(256 * ut, 128, stride=2), :] = n1
        state_o[pl.ds(256 * ut + 1, 128, stride=2), :] = n2

    for c in tw_c + x_c[0] + x_c[1] + a_c + q_c + g_c + y_c[0] + y_c[1]:
        c.wait_send()
    for c, sends, _ in cur_c + b1_c + p_c:
        pl.when(sends)(c.wait_send)
    for c in y_c[0] + y_c[1]:
        c.wait_recv()
    for c in own_y:
        c.wait()


def local_step(spectrum, time_weights, interp_weights, group_block, group_count, wave_state, neighbors, coupling):
    basis, own = host_basis()
    ws = wave_state.reshape(2, ROWS, 128).transpose(1, 0, 2).reshape(2 * ROWS, 128)
    cp = coupling.reshape(4, ROWS, 128).transpose(1, 0, 2).reshape(4 * ROWS, 128)
    hbm_spec = pl.BlockSpec(memory_space=pltpu.HBM)
    vmem_spec = pl.BlockSpec(memory_space=pltpu.VMEM)
    sem = pltpu.SemaphoreType.DMA
    spec = spectrum.reshape(2, FL, NBLK, BLK).transpose(1, 2, 0, 3).reshape(FL * 2 * NBLK, BLK)
    series, state = pl.pallas_call(
        kernel,
        out_shape=(pltpu.VMEM((TL, NP), F32), pltpu.VMEM((2 * ROWS, 128), F32)),
        in_specs=[hbm_spec] * 10,
        out_specs=(vmem_spec, vmem_spec),
        scratch_shapes=[
            pltpu.VMEM((FL * 2 * NBLK, BLK), F32),
            pltpu.VMEM((KP, NP), F32),
            pltpu.VMEM((2, TL), F32),
            pltpu.VMEM((FD, 2, TL), F32),
            pltpu.VMEM((16, 128), F32),
            pltpu.VMEM((2, 64, FD * 64), BF16),
            pltpu.VMEM((2, FD * KP, FD * KP), BF16),
            pltpu.VMEM((HALVES, FD * KP, HC), F32),
            pltpu.VMEM((HALVES, FD, TL, HC), F32),
            pltpu.VMEM((16 * NBLK, BLK), F32),
            pltpu.VMEM((FD, 64, BLK), F32),
            pltpu.VMEM((MD * SLOTS, BLK), F32),
            pltpu.VMEM((MD * SLOTS, BLK), F32),
            pltpu.VMEM((GROUPS, MD * SLOTS), BF16),
            pltpu.VMEM((MD, 2 * SLOTS, BLK), F32),
            pltpu.VMEM((MD, 2 * SLOTS, BLK), F32),
            pltpu.VMEM((GROUPS * BLK, BLK), F32),
            pltpu.VMEM((GROUPS * BLK, 2 * BLK), BF16),
            pltpu.VMEM((4, 512, EXT), BF16),
            pltpu.VMEM((2 * ROWS, 128), F32),
            pltpu.VMEM((4 * ROWS, 128), F32),
            pltpu.VMEM((4, ROWS), jnp.int32),
            pltpu.VMEM((1, 128), jnp.int32),
            pltpu.SMEM((1,), jnp.int32),
            pltpu.VMEM((2, HALO, 128), F32),
            pltpu.VMEM((2, HALO, 128), F32),
            pltpu.VMEM((2, HALO, 128), F32),
            pltpu.VMEM((HALO, 128), F32),
            pltpu.VMEM((HALO, 128), F32),
            pltpu.VMEM((EXT, 256), BF16),
            pltpu.VMEM((ROWS, 128), F32),
            pltpu.VMEM((ROWS, 128), F32),
            pltpu.VMEM((2, 4 * GROUPS, BLK), F32),
            pltpu.VMEM((4 * GROUPS, BLK), F32),
            sem((16,)),
            sem((FD,)), sem((FD,)),
            sem((HALVES, FD)), sem((HALVES, FD)),
            sem((FD,)), sem((FD,)),
            sem((MD,)), sem((MD,)),
            sem((MD,)), sem((MD,)),
            sem((6,)), sem((6,)),
            sem((HALVES, FD)), sem((HALVES, FD)),
            pltpu.SemaphoreType.REGULAR,
        ],
        compiler_params=pltpu.CompilerParams(
            collective_id=0, has_side_effects=True, vmem_limit_bytes=62 * 1024 * 1024
        ),
        name="p2o_wave",
    )(
        spec, time_weights, interp_weights.reshape(GROUPS * BLK, BLK), group_block.reshape(1, GROUPS),
        group_count, ws, neighbors, cp, jnp.asarray(basis), jnp.asarray(own),
    )
    new_state = state.reshape(ROWS, 2, 128).transpose(1, 0, 2).reshape(1, 2, ROWS * 128)
    return series, new_state


def solution(mesh):
    in_specs = (
        P(None, "freq", "mesh"),
        P(None, "freq"),
        P("mesh", None, None),
        P("mesh"),
        P("mesh"),
        P("freq", None, "mesh"),
        P(None, "mesh"),
        P(None, "mesh"),
    )
    out_specs = (P("freq", "mesh"), P("freq", None, "mesh"))
    return jax.shard_map(local_step, mesh=mesh, in_specs=in_specs, out_specs=out_specs, check_vma=False)
```

```python
import functools
import math

import jax
import jax.numpy as jnp
import numpy as np
from jax import lax
from jax.experimental import pallas as pl
from jax.experimental.pallas import tpu as pltpu
from jax.sharding import PartitionSpec as P

MESH = pl.DeviceIdType.MESH
F32 = jnp.float32
BF16 = jnp.bfloat16

NF = 216
NT = 432
FD = 8
MD = 16
FL = NF // FD
TL = NT // FD
KP = 56
NP = 4096
COLS = NP // FD
CHUNKS = ((0, 256), (256, 256))
BLK = 128
NBLK = NP // BLK
NHALF = NBLK // 2
GROUPS = 128
ROWS = 512
HALO = 32
EXT = 640
SLOTS = 8


def split_bf16(x):
    hi = x.astype(BF16)
    lo = (x - hi.astype(F32)).astype(BF16)
    return hi, lo


def host_split(x):
    hi = np.asarray(x, np.float32).astype(jnp.bfloat16)
    lo = (x - hi.astype(np.float64)).astype(jnp.bfloat16)
    return hi, lo


def host_basis():
    t = np.arange(NT)[:, None]
    k = np.arange(NF)[None, :]
    angle = (t * k % NT) * (2.0 * math.pi / NT)
    scale = np.where(k == 0, 1.0, 2.0) / NT
    full = np.zeros((FD, KP, FD, KP))
    full[:, :TL, :, :FL] = (np.cos(angle) * scale).reshape(FD, TL, FD, FL)
    full[:, :TL, :, FL : 2 * FL] = (-np.sin(angle) * scale).reshape(FD, TL, FD, FL)
    basis = np.stack(host_split(full.reshape(FD * KP, FD * KP)))
    own = np.zeros((FD, 64, FD, 64))
    own[:, :KP, :, :KP] = full.transpose(2, 1, 0, 3)
    own = own.reshape(FD, 64, FD * 64)
    return basis, np.stack(host_split(own), axis=1)


def dot(a, b):
    return jnp.dot(a, b, preferred_element_type=F32)


def dot_t(a, b):
    return lax.dot_general(a, b, (((1,), (1,)), ((), ())), preferred_element_type=F32)


def kernel(
    spec_h, tw_h, w_h, gb_h, gc_h, ws_h, nb_h, cp_h, basis_h, own_h,
    series_o, state_o,
    xs, xp, tws, twr, twf, cb, basis, r0, r1, s20, s21, pb, pr, ps, ra, rs, rq, pt, gs, gr, wf, whl, oh, ws, cp, nb, gb, gc,
    hs, hcur, hb1, hpush, hps, sb, base1, base2, lh, ee,
    lsem, tw_s, tw_r, x_s, x_r, a_s, a_r, q_s, q_r, g_s, g_r, h_s, h_r, y_s, y_r, mesh_sem,
):
    r, s2 = (r0, r1), (s20, s21)
    f = lax.axis_index("freq")
    m = lax.axis_index("mesh")

    def fdev(d):
        return (lax.rem(f + d, FD), m)

    def mdev(d):
        return (f, lax.rem(m + d, MD))

    def remote(src, dst, ssem, rsem, dev):
        return pltpu.make_async_remote_copy(
            src_ref=src, dst_ref=dst, send_sem=ssem, recv_sem=rsem, device_id=dev, device_id_type=MESH
        )

    bar = pltpu.get_barrier_semaphore()

    def tell(sem, dev):
        pl.semaphore_signal(sem, inc=1, device_id=dev, device_id_type=MESH)

    for d in range(1, FD):
        tell(bar, fdev(d))
    for d in range(1, MD):
        pl.when(m + d < MD)(functools.partial(tell, bar, mdev(d)))

    loads = [
        (spec_h, xs), (tw_h, tws), (own_h.at[f], cb), (nb_h, nb), (gb_h, gb), (gc_h, gc),
        (ws_h, ws), (cp_h, cp), (basis_h, basis), (w_h, wf),
    ]
    local = [pltpu.make_async_copy(s, d, lsem.at[i]) for i, (s, d) in enumerate(loads)]
    for c in local[:7]:
        c.start()

    twf[...] = jnp.zeros_like(twf)
    xp[KP - 8 :, :] = jnp.zeros((8, NP), F32)
    sb[ROWS:, :] = jnp.zeros((EXT - ROWS, 256), BF16)
    local[0].wait()
    for ct in range(NBLK):
        for part in range(2):
            xp[FL * part : FL * (part + 1), BLK * ct : BLK * (ct + 1)] = xs[pl.ds(2 * ct + part, FL, stride=2 * NBLK), :]
    local[1].wait()
    local[6].wait()
    hs[0] = ws[pl.ds(1, HALO, stride=2), :]
    hs[1] = ws[pl.ds(2 * (ROWS - HALO) + 1, HALO, stride=2), :]

    pl.semaphore_wait(bar, FD - 1 + m)

    tw_c = [remote(tws, twr.at[f], tw_s.at[d], tw_r.at[d], fdev(d)) for d in range(1, FD)]
    for c in tw_c:
        c.start()

    def cols_of(dev, h):
        first, width = CHUNKS[h]
        return pl.ds(pl.multiple_of(dev * COLS + first, 128), width)

    def x_copy(h, d):
        to = lax.rem(f + d, FD)
        rows = pl.ds(pl.multiple_of(f * KP, 8), KP)
        return remote(xp.at[:, cols_of(to, h)], r[h].at[rows], x_s.at[h, d], x_r.at[h, d], (to, m))

    x_c = [[x_copy(h, d) for d in range(1, FD)] for h in range(len(CHUNKS))]
    for c in x_c[0]:
        c.start()
    for d in range(1, MD):
        pl.when(m >= d)(functools.partial(tell, mesh_sem, mdev(MD - d)))
    for c in local[7:]:
        c.start()
    own_x = [
        pltpu.make_async_copy(
            xp.at[:, cols_of(f, h)], r[h].at[pl.ds(pl.multiple_of(f * KP, 8), KP)], lsem.at[10 + h]
        )
        for h in range(len(CHUNKS))
    ]
    for c in own_x:
        c.start()

    local[4].wait()
    local[5].wait()
    index = lax.broadcasted_iota(jnp.int32, (1, GROUPS), 1)
    live = index < gc[0]
    gbv = gb[...]
    owner = jnp.where(live, lax.shift_right_logical(gbv, 5), -1).astype(F32)
    inner = (lax.bitwise_and(gbv, NBLK - 1) + 1).astype(F32)
    lane_i = lax.broadcasted_iota(jnp.int32, (128, 128), 1)
    lane = lane_i.astype(F32)
    owner_r = jnp.broadcast_to(owner, (128, 128))
    owner_c = jnp.transpose(owner_r)
    earlier = lane_i < lax.broadcasted_iota(jnp.int32, (128, 128), 0)
    rank = jnp.sum(jnp.where(jnp.logical_and(owner_r == owner_c, earlier), 1.0, 0.0), axis=1, keepdims=True)
    slot = jnp.where(owner_c >= 0.0, owner_c * SLOTS + rank, -1.0)
    place = jnp.where(slot == lane, 1.0, 0.0)
    asked = jnp.sum(jnp.transpose(place) * inner, axis=1, keepdims=True) - 1.0
    rs[...] = jnp.broadcast_to(asked, (128, 128))
    pt[...] = place.astype(BF16)

    def q_copy(d):
        to = lax.rem(m + d, MD)
        src = rs.at[pl.ds(pl.multiple_of(to * SLOTS, 8), SLOTS)]
        dst = rq.at[pl.ds(pl.multiple_of(m * SLOTS, 8), SLOTS)]
        return remote(src, dst, q_s.at[d], q_r.at[d], (f, to))

    q_c = [q_copy(d) for d in range(1, MD)]
    rq[pl.ds(pl.multiple_of(m * SLOTS, 8), SLOTS), :] = rs[pl.ds(pl.multiple_of(m * SLOTS, 8), SLOTS), :]
    up, down = mdev(1), mdev(MD - 1)
    above, below = m < MD - 1, m > 0

    def halo_pair(i, low_src, high_src, dst):
        return [
            (remote(low_src, dst.at[1], h_s.at[i], h_r.at[i], down), below, above),
            (remote(high_src, dst.at[0], h_s.at[i + 1], h_r.at[i + 1], up), above, below),
        ]

    def start_all(pairs):
        for c, sends, _ in pairs:
            pl.when(sends)(functools.partial(c.start))

    def recv_all(pairs):
        for c, _, gets in pairs:
            pl.when(gets)(c.wait_recv)

    cur_c = halo_pair(0, hs.at[0], hs.at[1], hcur)

    def enter_mesh():
        pl.when(above)(lambda: pl.semaphore_wait(mesh_sem, MD - 1 - m))
        for c in q_c:
            c.start()
        start_all(cur_c)

    pl.when(m >= MD // 2)(enter_mesh)

    local[2].wait()
    for c in tw_c:
        c.wait_recv()
    twr[f] = tws[...]
    for w in range(FD):
        twf[2 * w : 2 * w + 2, 0:TL] = twr[w]
    th, tl = split_bf16(twf[:, 0:64])
    g_all = dot(th, cb[0]) + dot(tl, cb[0]) + dot(th, cb[1])
    row_w = lax.broadcasted_iota(jnp.int32, (16, 128), 0) // 2
    lane_w = lax.broadcasted_iota(jnp.int32, (16, 128), 1) // 64
    g2 = jnp.zeros((16, 128), F32)
    for i in range(4):
        g2 = g2 + jnp.where(lane_w + 2 * i == row_w, g_all[:, 128 * i : 128 * (i + 1)], 0.0)
    g = (g2 + pltpu.roll(g2, 64, 1))[:, 0:KP]
    gh, gl = split_bf16(g)
    ghl = jnp.concatenate([gh, gl], axis=0)
    for q in range(8):
        xh, xl = split_bf16(xp[:, 512 * q : 512 * (q + 1)])
        both = dot(ghl, xh)
        part = both[0:16] + both[16:32] + dot(gh, xl)
        for b in range(4):
            pb[q // 4, pl.ds(4 * (q % 4) + b, 16, stride=NHALF), :] = part[:, 128 * b : 128 * (b + 1)]

    core = lax.rem(f, 2)
    pair_c = remote(pb.at[1 - core], pr, a_s.at[0], a_r.at[0], (f + 1 - 2 * core, m))
    pair_c.start()
    pair_c.wait_recv()
    ps[...] = pb[core] + pr[...]

    def a_copy(d):
        to = lax.rem(f + d, FD)
        src = ps.at[pl.ds(pl.multiple_of(to * 2 * NHALF, 8), 2 * NHALF)]
        return remote(src, ra.at[f], a_s.at[d], a_r.at[d], (to, m))

    a_c = [a_copy(d) for d in range(1, FD)]
    for c in a_c:
        c.start()
    for c in x_c[1]:
        c.start()
    ra[f] = ps[pl.ds(pl.multiple_of(f * 2 * NHALF, 8), 2 * NHALF), :]

    local[3].wait()
    nbv = nb[...]
    nbv = jnp.where(nbv >= ROWS + HALO, nbv, jnp.where(nbv < HALO, nbv + ROWS, nbv - HALO)).astype(F32)
    for n in range(4):
        for ut in range(4):
            col = jnp.transpose(jnp.broadcast_to(nbv[n : n + 1, 128 * ut : 128 * (ut + 1)], (128, 128)))
            for kt in range(EXT // 128):
                hot = jnp.where(col == lane + float(128 * kt), 1.0, 0.0).astype(BF16)
                oh[ut, 128 * n : 128 * (n + 1), 128 * kt : 128 * (kt + 1)] = hot

    local[9].wait()

    def split_w(i, carry):
        rows = pl.ds(pl.multiple_of(i * 512, 512), 512)
        hi, lo = split_bf16(wf[rows, :])
        whl[rows, 0:128] = hi
        whl[rows, 128:256] = lo
        return carry

    lax.fori_loop(0, GROUPS * BLK // 512, split_w, 0)

    pl.when(m < MD // 2)(enter_mesh)

    local[8].wait()

    def y_copy(h, d):
        to = lax.rem(f + d, FD)
        return remote(s2[h].at[to], series_o.at[:, cols_of(f, h)], y_s.at[h, d], y_r.at[h, d], (to, m))

    y_c = [[y_copy(h, d) for d in range(1, FD)] for h in range(len(CHUNKS))]
    own_y = []

    def transform(h):
        for c in x_c[h]:
            c.wait_recv()
        own_x[h].wait()
        xh, xl = split_bf16(r[h][...])
        out = dot(basis[0], xh) + dot(basis[0], xl) + dot(basis[1], xh)
        for w in range(FD):
            s2[h][w] = out[KP * w : KP * w + TL]
        for c in y_c[h]:
            c.start()
        c = pltpu.make_async_copy(
            s2[h].at[f], series_o.at[:, cols_of(f, h)], lsem.at[12 + h]
        )
        c.start()
        own_y.append(c)


    transform(0)

    for c in q_c:
        c.wait_recv()
    sel = jnp.where(rq[...] == lane, 1.0, 0.0).astype(BF16)[:, 0:NBLK]
    for c in a_c:
        c.wait_recv()
    total = [ra[c] + ra[2 + c] + ra[4 + c] + ra[6 + c] for c in range(2)]
    for s in range(2):
        rows = slice(NHALF * s, NHALF * (s + 1))
        hi, lo = split_bf16(jnp.concatenate([total[0][rows], total[1][rows]], axis=0))
        out = dot(sel, hi) + dot(sel, lo)
        for o in range(MD):
            gs[o, SLOTS * s : SLOTS * (s + 1), :] = out[SLOTS * o : SLOTS * (o + 1)]

    def g_copy(d):
        to = lax.rem(m + d, MD)
        return remote(gs.at[to], gr.at[m], g_s.at[d], g_r.at[d], (f, to))

    g_c = [g_copy(d) for d in range(1, MD)]
    for c in g_c:
        c.start()
    gr[m] = gs[m]

    transform(1)

    for i in (7,):
        local[i].wait()

    def put_ext(lo_row, value):
        hi, lo = split_bf16(value)
        sb[lo_row : lo_row + value.shape[0], 0:128] = hi
        sb[lo_row : lo_row + value.shape[0], 128:256] = lo

    def put_halo(buf):
        put_ext(ROWS, jnp.where(m > 0, buf[0], 0.0))
        put_ext(ROWS + HALO, jnp.where(m < MD - 1, buf[1], 0.0))

    def spread(ut, v):
        e = dot(oh[ut], sb[...])
        total = jnp.zeros((128, 128), F32)
        for n in range(4):
            c = cp[pl.ds(512 * ut + n, 128, stride=4), :]
            total = total + c * (e[128 * n : 128 * (n + 1), 0:128] + e[128 * n : 128 * (n + 1), 128:256] - v)
        return total

    put_ext(0, ws[pl.ds(1, ROWS, stride=2), :])
    recv_all(cur_c)
    put_halo(hcur)
    for ut in range(4):
        cur = ws[pl.ds(256 * ut + 1, 128, stride=2), :]
        prev = ws[pl.ds(256 * ut, 128, stride=2), :]
        base1[128 * ut : 128 * (ut + 1), :] = 2.0 * cur - prev + spread(ut, cur)
    b1_c = halo_pair(2, base1.at[0:HALO], base1.at[ROWS - HALO : ROWS], hb1)
    start_all(b1_c)

    for c in g_c:
        c.wait_recv()
    for s in range(2):
        blocks = gr[:, SLOTS * s : SLOTS * (s + 1), :].reshape(MD * SLOTS, BLK)
        hi, lo = split_bf16(blocks)
        ph = dot(pt[...], hi)
        lh[0, pl.ds(2 * s, 128, stride=4), :] = ph
        lh[1, pl.ds(2 * s, 128, stride=4), :] = ph
        lh[0, pl.ds(2 * s + 1, 128, stride=4), :] = dot(pt[...], lo)
        lh[1, pl.ds(2 * s + 1, 128, stride=4), :] = jnp.zeros((128, 128), F32)
    upper = lax.broadcasted_iota(jnp.int32, (8, 128), 0) < 4

    def interp(i, carry):
        for j in range(16):
            rows = pl.ds(pl.multiple_of(i * 128 + 8 * j, 8), 8)
            w = whl[pl.ds(pl.multiple_of(i * 4096 + 256 * j, 256), 256), :]
            left = jnp.concatenate([lh[0, rows, :], lh[1, rows, :]], axis=1).astype(BF16)
            out = dot_t(left, w)
            ee[rows, :] = jnp.where(upper, out[:, 0:128], out[:, 128:256])
        return carry

    lax.fori_loop(0, GROUPS // 32, interp, 0)
    push0 = ee[pl.ds(0, 128, stride=4), :] + ee[pl.ds(1, 128, stride=4), :]
    push1 = ee[pl.ds(2, 128, stride=4), :] + ee[pl.ds(3, 128, stride=4), :]
    hps[...] = push0[0:HALO]
    p_c = [(remote(hps, hpush, h_s.at[4], h_r.at[4], down), below, above)]
    start_all(p_c)

    put_ext(0, base1[...])
    recv_all(b1_c)
    put_halo(hb1)
    for ut in range(4):
        cur = ws[pl.ds(256 * ut + 1, 128, stride=2), :]
        b1 = base1[128 * ut : 128 * (ut + 1), :]
        base2[128 * ut : 128 * (ut + 1), :] = 2.0 * b1 - cur + spread(ut, b1)

    sb[ROWS : ROWS + HALO, :] = jnp.zeros((HALO, 256), BF16)
    put_ext(0, push0)
    recv_all(p_c)
    put_ext(ROWS + HALO, jnp.where(m < MD - 1, hpush[...], 0.0))
    for ut in range(4):
        e = dot(oh[ut, :, 0:128], sb[0:128, :]) + dot(oh[ut, :, ROWS:EXT], sb[ROWS:EXT, :])
        total = jnp.zeros((128, 128), F32)
        for n in range(4):
            c = cp[pl.ds(512 * ut + n, 128, stride=4), :]
            en = e[128 * n : 128 * (n + 1), 0:128] + e[128 * n : 128 * (n + 1), 128:256]
            total = total + c * (en - push0 if ut == 0 else en)
        n1 = base1[128 * ut : 128 * (ut + 1), :]
        n2 = base2[128 * ut : 128 * (ut + 1), :] + total
        if ut == 0:
            n1 = n1 + push0
            n2 = n2 + 2.0 * push0 + push1
        state_o[pl.ds(256 * ut, 128, stride=2), :] = n1
        state_o[pl.ds(256 * ut + 1, 128, stride=2), :] = n2

    for c in [pair_c] + tw_c + x_c[0] + x_c[1] + a_c + q_c + g_c + y_c[0] + y_c[1]:
        c.wait_send()
    for c, sends, _ in cur_c + b1_c + p_c:
        pl.when(sends)(c.wait_send)
    for c in y_c[0] + y_c[1]:
        c.wait_recv()
    for c in own_y:
        c.wait()


def write_out(series, state, series_o, state_o, sem):
    copies = [pltpu.make_async_copy(series, series_o, sem.at[0]), pltpu.make_async_copy(state, state_o, sem.at[1])]
    for c in copies:
        c.start()
    for c in copies:
        c.wait()


def local_step(spectrum, time_weights, interp_weights, group_block, group_count, wave_state, neighbors, coupling):
    basis, own = host_basis()
    ws = wave_state.reshape(2, ROWS, 128).transpose(1, 0, 2).reshape(2 * ROWS, 128)
    cp = coupling.reshape(4, ROWS, 128).transpose(1, 0, 2).reshape(4 * ROWS, 128)
    hbm_spec = pl.BlockSpec(memory_space=pltpu.HBM)
    vmem_spec = pl.BlockSpec(memory_space=pltpu.VMEM)
    sem = pltpu.SemaphoreType.DMA
    spec = spectrum.reshape(2, FL, NBLK, BLK).transpose(1, 2, 0, 3).reshape(FL * 2 * NBLK, BLK)
    series, state = pl.pallas_call(
        kernel,
        out_shape=(pltpu.VMEM((TL, NP), F32), pltpu.VMEM((2 * ROWS, 128), F32)),
        in_specs=[hbm_spec] * 10,
        out_specs=(vmem_spec, vmem_spec),
        scratch_shapes=[
            pltpu.VMEM((FL * 2 * NBLK, BLK), F32),
            pltpu.VMEM((KP, NP), F32),
            pltpu.VMEM((2, TL), F32),
            pltpu.VMEM((FD, 2, TL), F32),
            pltpu.VMEM((16, 128), F32),
            pltpu.VMEM((2, 64, FD * 64), BF16),
            pltpu.VMEM((2, FD * KP, FD * KP), BF16),
            *[pltpu.VMEM((FD * KP, width), F32) for _, width in CHUNKS],
            *[pltpu.VMEM((FD, TL, width), F32) for _, width in CHUNKS],
            pltpu.VMEM((2, 16 * NHALF, BLK), F32),
            pltpu.VMEM((16 * NHALF, BLK), F32),
            pltpu.VMEM((16 * NHALF, BLK), F32),
            pltpu.VMEM((FD, 2 * NHALF, BLK), F32),
            pltpu.VMEM((MD * SLOTS, BLK), F32),
            pltpu.VMEM((MD * SLOTS, BLK), F32),
            pltpu.VMEM((GROUPS, MD * SLOTS), BF16),
            pltpu.VMEM((MD, 2 * SLOTS, BLK), F32),
            pltpu.VMEM((MD, 2 * SLOTS, BLK), F32),
            pltpu.VMEM((GROUPS * BLK, BLK), F32),
            pltpu.VMEM((GROUPS * BLK, 2 * BLK), BF16),
            pltpu.VMEM((4, 512, EXT), BF16),
            pltpu.VMEM((2 * ROWS, 128), F32),
            pltpu.VMEM((4 * ROWS, 128), F32),
            pltpu.VMEM((4, ROWS), jnp.int32),
            pltpu.VMEM((1, 128), jnp.int32),
            pltpu.SMEM((1,), jnp.int32),
            pltpu.VMEM((2, HALO, 128), F32),
            pltpu.VMEM((2, HALO, 128), F32),
            pltpu.VMEM((2, HALO, 128), F32),
            pltpu.VMEM((HALO, 128), F32),
            pltpu.VMEM((HALO, 128), F32),
            pltpu.VMEM((EXT, 256), BF16),
            pltpu.VMEM((ROWS, 128), F32),
            pltpu.VMEM((ROWS, 128), F32),
            pltpu.VMEM((2, 4 * GROUPS, BLK), F32),
            pltpu.VMEM((4 * GROUPS, BLK), F32),
            sem((16,)),
            sem((FD,)), sem((FD,)),
            sem((len(CHUNKS), FD)), sem((len(CHUNKS), FD)),
            sem((FD,)), sem((FD,)),
            sem((MD,)), sem((MD,)),
            sem((MD,)), sem((MD,)),
            sem((6,)), sem((6,)),
            sem((len(CHUNKS), FD)), sem((len(CHUNKS), FD)),
            pltpu.SemaphoreType.REGULAR,
        ],
        compiler_params=pltpu.CompilerParams(
            collective_id=0, has_side_effects=True, vmem_limit_bytes=62 * 1024 * 1024
        ),
        name="p2o_wave",
    )(
        spec, time_weights, interp_weights.reshape(GROUPS * BLK, BLK), group_block.reshape(1, GROUPS),
        group_count, ws, neighbors, cp, jnp.asarray(basis), jnp.asarray(own),
    )
    series, state = pl.pallas_call(
        write_out,
        out_shape=(jax.ShapeDtypeStruct((TL, NP), F32), jax.ShapeDtypeStruct((2 * ROWS, 128), F32)),
        in_specs=[pl.BlockSpec(memory_space=pltpu.VMEM)] * 2,
        out_specs=(hbm_spec, hbm_spec),
        scratch_shapes=[sem((2,))],
        name="write_out",
    )(pltpu.with_memory_space_constraint(series, pltpu.VMEM), pltpu.with_memory_space_constraint(state, pltpu.VMEM))
    new_state = state.reshape(ROWS, 2, 128).transpose(1, 0, 2).reshape(1, 2, ROWS * 128)
    return series, new_state


def solution(mesh):
    in_specs = (
        P(None, "freq", "mesh"),
        P(None, "freq"),
        P("mesh", None, None),
        P("mesh"),
        P("mesh"),
        P("freq", None, "mesh"),
        P(None, "mesh"),
        P(None, "mesh"),
    )
    out_specs = (P("freq", "mesh"), P("freq", None, "mesh"))
    return jax.shard_map(local_step, mesh=mesh, in_specs=in_specs, out_specs=out_specs, check_vma=False)
```

```python
import functools
import math

import jax
import jax.numpy as jnp
import numpy as np
from jax import lax
from jax.experimental import pallas as pl
from jax.experimental.pallas import tpu as pltpu
from jax.sharding import PartitionSpec as P

MESH = pl.DeviceIdType.MESH
F32 = jnp.float32
BF16 = jnp.bfloat16

NF = 216
NT = 432
FD = 8
MD = 16
FL = NF // FD
TL = NT // FD
KP = 56
NP = 4096
COLS = NP // FD
CHUNKS = ((0, 256), (256, 128), (384, 128))
EARLY = 2
BLK = 128
NBLK = NP // BLK
NHALF = NBLK // 2
GROUPS = 128
ROWS = 512
HALO = 32
EXT = 640
SLOTS = 8


def split_bf16(x):
    hi = x.astype(BF16)
    lo = (x - hi.astype(F32)).astype(BF16)
    return hi, lo


def host_split(x):
    hi = np.asarray(x, np.float32).astype(jnp.bfloat16)
    lo = (x - hi.astype(np.float64)).astype(jnp.bfloat16)
    return hi, lo


def host_basis():
    t = np.arange(NT)[:, None]
    k = np.arange(NF)[None, :]
    angle = (t * k % NT) * (2.0 * math.pi / NT)
    scale = np.where(k == 0, 1.0, 2.0) / NT
    full = np.zeros((FD, KP, FD, KP))
    full[:, :TL, :, :FL] = (np.cos(angle) * scale).reshape(FD, TL, FD, FL)
    full[:, :TL, :, FL : 2 * FL] = (-np.sin(angle) * scale).reshape(FD, TL, FD, FL)
    basis = np.stack(host_split(full.reshape(FD * KP, FD * KP)))
    own = np.zeros((FD, 64, FD, 64))
    own[:, :KP, :, :KP] = full.transpose(2, 1, 0, 3)
    own = own.reshape(FD, 64, FD * 64)
    return basis, np.stack(host_split(own), axis=1)


def dot(a, b):
    return jnp.dot(a, b, preferred_element_type=F32)


def dot_t(a, b):
    return lax.dot_general(a, b, (((1,), (1,)), ((), ())), preferred_element_type=F32)


def kernel(
    spec_h, tw_h, w_h, gb_h, gc_h, ws_h, nb_h, cp_h, basis_h, own_h,
    series_o, state_o,
    xs, xp, tws, twr, twf, cb, basis, r0, r1, r2, s20, s21, s22, pb, pr, ps, ra, rs, rq, pt, gs, gr, wf, whl, oh, ws, cp, nb, gb, gc,
    hs, hcur, hb1, hpush, hps, sb, base1, base2, lh, ee,
    lsem, tw_s, tw_r, x_s, x_r, a_s, a_r, q_s, q_r, g_s, g_r, h_s, h_r, y_s, y_r, mesh_sem,
):
    r = (r0, r1, r2)
    s2 = (s20, s21, s22)
    f = lax.axis_index("freq")
    m = lax.axis_index("mesh")

    def fdev(d):
        return (lax.rem(f + d, FD), m)

    def mdev(d):
        return (f, lax.rem(m + d, MD))

    def remote(src, dst, ssem, rsem, dev):
        return pltpu.make_async_remote_copy(
            src_ref=src, dst_ref=dst, send_sem=ssem, recv_sem=rsem, device_id=dev, device_id_type=MESH
        )

    bar = pltpu.get_barrier_semaphore()

    def tell(sem, dev):
        pl.semaphore_signal(sem, inc=1, device_id=dev, device_id_type=MESH)

    for d in range(1, FD):
        tell(bar, fdev(d))
    for d in range(1, MD):
        pl.when(m + d < MD)(functools.partial(tell, bar, mdev(d)))

    loads = [
        (spec_h, xs), (tw_h, tws), (own_h.at[f], cb), (nb_h, nb), (gb_h, gb), (gc_h, gc),
        (ws_h, ws), (cp_h, cp), (basis_h, basis), (w_h, wf),
    ]
    local = [pltpu.make_async_copy(s, d, lsem.at[i]) for i, (s, d) in enumerate(loads)]
    for c in local[:7]:
        c.start()

    twf[...] = jnp.zeros_like(twf)
    xp[KP - 8 :, :] = jnp.zeros((8, NP), F32)
    sb[ROWS:, :] = jnp.zeros((EXT - ROWS, 256), BF16)
    local[0].wait()
    for ct in range(NBLK):
        for part in range(2):
            xp[FL * part : FL * (part + 1), BLK * ct : BLK * (ct + 1)] = xs[pl.ds(2 * ct + part, FL, stride=2 * NBLK), :]
    local[1].wait()
    local[6].wait()
    hs[0] = ws[pl.ds(1, HALO, stride=2), :]
    hs[1] = ws[pl.ds(2 * (ROWS - HALO) + 1, HALO, stride=2), :]

    pl.semaphore_wait(bar, FD - 1 + m)

    tw_c = [remote(tws, twr.at[f], tw_s.at[d], tw_r.at[d], fdev(d)) for d in range(1, FD)]
    for c in tw_c:
        c.start()

    def cols_of(dev, h):
        first, width = CHUNKS[h]
        return pl.ds(pl.multiple_of(dev * COLS + first, 128), width)

    def x_copy(h, d):
        to = lax.rem(f + d, FD)
        rows = pl.ds(pl.multiple_of(f * KP, 8), KP)
        return remote(xp.at[:, cols_of(to, h)], r[h].at[rows], x_s.at[h, d], x_r.at[h, d], (to, m))

    x_c = [[x_copy(h, d) for d in range(1, FD)] for h in range(len(CHUNKS))]
    for h in range(EARLY):
        for c in x_c[h]:
            c.start()
    for d in range(1, MD):
        pl.when(m >= d)(functools.partial(tell, mesh_sem, mdev(MD - d)))
    for c in local[7:]:
        c.start()
    own_x = [
        pltpu.make_async_copy(
            xp.at[:, cols_of(f, h)], r[h].at[pl.ds(pl.multiple_of(f * KP, 8), KP)], lsem.at[10 + h]
        )
        for h in range(len(CHUNKS))
    ]
    for c in own_x:
        c.start()

    local[4].wait()
    local[5].wait()
    index = lax.broadcasted_iota(jnp.int32, (1, GROUPS), 1)
    live = index < gc[0]
    gbv = gb[...]
    owner = jnp.where(live, lax.shift_right_logical(gbv, 5), -1).astype(F32)
    inner = (lax.bitwise_and(gbv, NBLK - 1) + 1).astype(F32)
    lane_i = lax.broadcasted_iota(jnp.int32, (128, 128), 1)
    lane = lane_i.astype(F32)
    owner_r = jnp.broadcast_to(owner, (128, 128))
    owner_c = jnp.transpose(owner_r)
    earlier = lane_i < lax.broadcasted_iota(jnp.int32, (128, 128), 0)
    rank = jnp.sum(jnp.where(jnp.logical_and(owner_r == owner_c, earlier), 1.0, 0.0), axis=1, keepdims=True)
    slot = jnp.where(owner_c >= 0.0, owner_c * SLOTS + rank, -1.0)
    place = jnp.where(slot == lane, 1.0, 0.0)
    asked = jnp.sum(jnp.transpose(place) * inner, axis=1, keepdims=True) - 1.0
    rs[...] = jnp.broadcast_to(asked, (128, 128))
    pt[...] = place.astype(BF16)

    def q_copy(d):
        to = lax.rem(m + d, MD)
        src = rs.at[pl.ds(pl.multiple_of(to * SLOTS, 8), SLOTS)]
        dst = rq.at[pl.ds(pl.multiple_of(m * SLOTS, 8), SLOTS)]
        return remote(src, dst, q_s.at[d], q_r.at[d], (f, to))

    q_c = [q_copy(d) for d in range(1, MD)]
    rq[pl.ds(pl.multiple_of(m * SLOTS, 8), SLOTS), :] = rs[pl.ds(pl.multiple_of(m * SLOTS, 8), SLOTS), :]
    up, down = mdev(1), mdev(MD - 1)
    above, below = m < MD - 1, m > 0

    def halo_pair(i, low_src, high_src, dst):
        return [
            (remote(low_src, dst.at[1], h_s.at[i], h_r.at[i], down), below, above),
            (remote(high_src, dst.at[0], h_s.at[i + 1], h_r.at[i + 1], up), above, below),
        ]

    def start_all(pairs):
        for c, sends, _ in pairs:
            pl.when(sends)(functools.partial(c.start))

    def recv_all(pairs):
        for c, _, gets in pairs:
            pl.when(gets)(c.wait_recv)

    cur_c = halo_pair(0, hs.at[0], hs.at[1], hcur)

    def enter_mesh():
        pl.when(above)(lambda: pl.semaphore_wait(mesh_sem, MD - 1 - m))
        for c in q_c:
            c.start()
        start_all(cur_c)

    pl.when(m >= MD // 2)(enter_mesh)

    local[2].wait()
    for c in tw_c:
        c.wait_recv()
    twr[f] = tws[...]
    for w in range(FD):
        twf[2 * w : 2 * w + 2, 0:TL] = twr[w]
    th, tl = split_bf16(twf[:, 0:64])
    g_all = dot(th, cb[0]) + dot(tl, cb[0]) + dot(th, cb[1])
    row_w = lax.broadcasted_iota(jnp.int32, (16, 128), 0) // 2
    lane_w = lax.broadcasted_iota(jnp.int32, (16, 128), 1) // 64
    g2 = jnp.zeros((16, 128), F32)
    for i in range(4):
        g2 = g2 + jnp.where(lane_w + 2 * i == row_w, g_all[:, 128 * i : 128 * (i + 1)], 0.0)
    g = (g2 + pltpu.roll(g2, 64, 1))[:, 0:KP]
    gh, gl = split_bf16(g)
    ghl = jnp.concatenate([gh, gl], axis=0)
    for q in range(8):
        xh, xl = split_bf16(xp[:, 512 * q : 512 * (q + 1)])
        both = dot(ghl, xh)
        part = both[0:16] + both[16:32] + dot(gh, xl)
        for b in range(4):
            pb[q // 4, pl.ds(4 * (q % 4) + b, 16, stride=NHALF), :] = part[:, 128 * b : 128 * (b + 1)]

    core = lax.rem(f, 2)
    pair_c = remote(pb.at[1 - core], pr, a_s.at[0], a_r.at[0], (f + 1 - 2 * core, m))
    pair_c.start()
    pair_c.wait_recv()
    ps[...] = pb[core] + pr[...]

    def a_copy(d):
        to = lax.rem(f + d, FD)
        src = ps.at[pl.ds(pl.multiple_of(to * 2 * NHALF, 8), 2 * NHALF)]
        return remote(src, ra.at[f], a_s.at[d], a_r.at[d], (to, m))

    a_c = [a_copy(d) for d in range(1, FD)]
    for c in a_c:
        c.start()
    for h in range(EARLY, len(CHUNKS)):
        for c in x_c[h]:
            c.start()
    ra[f] = ps[pl.ds(pl.multiple_of(f * 2 * NHALF, 8), 2 * NHALF), :]

    local[3].wait()
    nbv = nb[...]
    nbv = jnp.where(nbv >= ROWS + HALO, nbv, jnp.where(nbv < HALO, nbv + ROWS, nbv - HALO)).astype(F32)
    for n in range(4):
        for ut in range(4):
            col = jnp.transpose(jnp.broadcast_to(nbv[n : n + 1, 128 * ut : 128 * (ut + 1)], (128, 128)))
            for kt in range(EXT // 128):
                hot = jnp.where(col == lane + float(128 * kt), 1.0, 0.0).astype(BF16)
                oh[ut, 128 * n : 128 * (n + 1), 128 * kt : 128 * (kt + 1)] = hot

    local[9].wait()

    def split_w(i, carry):
        rows = pl.ds(pl.multiple_of(i * 512, 512), 512)
        hi, lo = split_bf16(wf[rows, :])
        whl[rows, 0:128] = hi
        whl[rows, 128:256] = lo
        return carry

    lax.fori_loop(0, GROUPS * BLK // 512, split_w, 0)

    pl.when(m < MD // 2)(enter_mesh)

    local[8].wait()

    def y_copy(h, d):
        to = lax.rem(f + d, FD)
        return remote(s2[h].at[to], series_o.at[:, cols_of(f, h)], y_s.at[h, d], y_r.at[h, d], (to, m))

    y_c = [[y_copy(h, d) for d in range(1, FD)] for h in range(len(CHUNKS))]
    own_y = []

    def transform(h):
        for c in x_c[h]:
            c.wait_recv()
        own_x[h].wait()
        xh, xl = split_bf16(r[h][...])
        out = dot(basis[0], xh) + dot(basis[0], xl) + dot(basis[1], xh)
        for w in range(FD):
            s2[h][w] = out[KP * w : KP * w + TL]
        for c in y_c[h]:
            c.start()
        c = pltpu.make_async_copy(
            s2[h].at[f], series_o.at[:, cols_of(f, h)], lsem.at[13 + h]
        )
        c.start()
        own_y.append(c)


    transform(0)

    for c in q_c:
        c.wait_recv()
    sel = jnp.where(rq[...] == lane, 1.0, 0.0).astype(BF16)[:, 0:NBLK]
    for c in a_c:
        c.wait_recv()
    total = [ra[c] + ra[2 + c] + ra[4 + c] + ra[6 + c] for c in range(2)]
    for s in range(2):
        rows = slice(NHALF * s, NHALF * (s + 1))
        hi, lo = split_bf16(jnp.concatenate([total[0][rows], total[1][rows]], axis=0))
        out = dot(sel, hi) + dot(sel, lo)
        for o in range(MD):
            gs[o, SLOTS * s : SLOTS * (s + 1), :] = out[SLOTS * o : SLOTS * (o + 1)]

    def g_copy(d):
        to = lax.rem(m + d, MD)
        return remote(gs.at[to], gr.at[m], g_s.at[d], g_r.at[d], (f, to))

    g_c = [g_copy(d) for d in range(1, MD)]
    for c in g_c:
        c.start()
    gr[m] = gs[m]

    for i in (7,):
        local[i].wait()

    def put_ext(lo_row, value):
        hi, lo = split_bf16(value)
        sb[lo_row : lo_row + value.shape[0], 0:128] = hi
        sb[lo_row : lo_row + value.shape[0], 128:256] = lo

    def put_halo(buf):
        put_ext(ROWS, jnp.where(m > 0, buf[0], 0.0))
        put_ext(ROWS + HALO, jnp.where(m < MD - 1, buf[1], 0.0))

    def spread(ut, v):
        e = dot(oh[ut], sb[...])
        total = jnp.zeros((128, 128), F32)
        for n in range(4):
            c = cp[pl.ds(512 * ut + n, 128, stride=4), :]
            total = total + c * (e[128 * n : 128 * (n + 1), 0:128] + e[128 * n : 128 * (n + 1), 128:256] - v)
        return total

    put_ext(0, ws[pl.ds(1, ROWS, stride=2), :])
    recv_all(cur_c)
    put_halo(hcur)
    for ut in range(4):
        cur = ws[pl.ds(256 * ut + 1, 128, stride=2), :]
        prev = ws[pl.ds(256 * ut, 128, stride=2), :]
        base1[128 * ut : 128 * (ut + 1), :] = 2.0 * cur - prev + spread(ut, cur)
    b1_c = halo_pair(2, base1.at[0:HALO], base1.at[ROWS - HALO : ROWS], hb1)
    start_all(b1_c)

    transform(1)
    transform(2)

    put_ext(0, base1[...])
    recv_all(b1_c)
    put_halo(hb1)
    for ut in range(4):
        cur = ws[pl.ds(256 * ut + 1, 128, stride=2), :]
        b1 = base1[128 * ut : 128 * (ut + 1), :]
        base2[128 * ut : 128 * (ut + 1), :] = 2.0 * b1 - cur + spread(ut, b1)

    for c in g_c:
        c.wait_recv()
    for s in range(2):
        blocks = gr[:, SLOTS * s : SLOTS * (s + 1), :].reshape(MD * SLOTS, BLK)
        hi, lo = split_bf16(blocks)
        ph = dot(pt[...], hi)
        lh[0, pl.ds(2 * s, 128, stride=4), :] = ph
        lh[1, pl.ds(2 * s, 128, stride=4), :] = ph
        lh[0, pl.ds(2 * s + 1, 128, stride=4), :] = dot(pt[...], lo)
        lh[1, pl.ds(2 * s + 1, 128, stride=4), :] = jnp.zeros((128, 128), F32)
    upper = lax.broadcasted_iota(jnp.int32, (8, 128), 0) < 4

    def interp(i, carry):
        for j in range(16):
            rows = pl.ds(pl.multiple_of(i * 128 + 8 * j, 8), 8)
            w = whl[pl.ds(pl.multiple_of(i * 4096 + 256 * j, 256), 256), :]
            left = jnp.concatenate([lh[0, rows, :], lh[1, rows, :]], axis=1).astype(BF16)
            out = dot_t(left, w)
            ee[rows, :] = jnp.where(upper, out[:, 0:128], out[:, 128:256])
        return carry

    interp(0, 0)
    hps[...] = ee[pl.ds(0, HALO, stride=4), :] + ee[pl.ds(1, HALO, stride=4), :]
    p_c = [(remote(hps, hpush, h_s.at[4], h_r.at[4], down), below, above)]
    start_all(p_c)
    for i in range(1, GROUPS // 32):
        interp(i, 0)
    push0 = ee[pl.ds(0, 128, stride=4), :] + ee[pl.ds(1, 128, stride=4), :]
    push1 = ee[pl.ds(2, 128, stride=4), :] + ee[pl.ds(3, 128, stride=4), :]

    sb[ROWS : ROWS + HALO, :] = jnp.zeros((HALO, 256), BF16)
    put_ext(0, push0)
    recv_all(p_c)
    put_ext(ROWS + HALO, jnp.where(m < MD - 1, hpush[...], 0.0))
    for ut in range(4):
        e = dot(oh[ut, :, 0:128], sb[0:128, :]) + dot(oh[ut, :, ROWS:EXT], sb[ROWS:EXT, :])
        total = jnp.zeros((128, 128), F32)
        for n in range(4):
            c = cp[pl.ds(512 * ut + n, 128, stride=4), :]
            en = e[128 * n : 128 * (n + 1), 0:128] + e[128 * n : 128 * (n + 1), 128:256]
            total = total + c * (en - push0 if ut == 0 else en)
        n1 = base1[128 * ut : 128 * (ut + 1), :]
        n2 = base2[128 * ut : 128 * (ut + 1), :] + total
        if ut == 0:
            n1 = n1 + push0
            n2 = n2 + 2.0 * push0 + push1
        state_o[pl.ds(256 * ut, 128, stride=2), :] = n1
        state_o[pl.ds(256 * ut + 1, 128, stride=2), :] = n2

    for c in [pair_c] + tw_c + sum(x_c, []) + a_c + q_c + g_c + sum(y_c, []):
        c.wait_send()
    for c, sends, _ in cur_c + b1_c + p_c:
        pl.when(sends)(c.wait_send)
    for c in sum(y_c, []):
        c.wait_recv()
    for c in own_y:
        c.wait()


def write_out(series, state, series_o, state_o, sem):
    copies = [pltpu.make_async_copy(series, series_o, sem.at[0]), pltpu.make_async_copy(state, state_o, sem.at[1])]
    for c in copies:
        c.start()
    for c in copies:
        c.wait()


def local_step(spectrum, time_weights, interp_weights, group_block, group_count, wave_state, neighbors, coupling):
    basis, own = host_basis()
    ws = wave_state.reshape(2, ROWS, 128).transpose(1, 0, 2).reshape(2 * ROWS, 128)
    cp = coupling.reshape(4, ROWS, 128).transpose(1, 0, 2).reshape(4 * ROWS, 128)
    hbm_spec = pl.BlockSpec(memory_space=pltpu.HBM)
    vmem_spec = pl.BlockSpec(memory_space=pltpu.VMEM)
    sem = pltpu.SemaphoreType.DMA
    spec = spectrum.reshape(2, FL, NBLK, BLK).transpose(1, 2, 0, 3).reshape(FL * 2 * NBLK, BLK)
    series, state = pl.pallas_call(
        kernel,
        out_shape=(pltpu.VMEM((TL, NP), F32), pltpu.VMEM((2 * ROWS, 128), F32)),
        in_specs=[hbm_spec] * 10,
        out_specs=(vmem_spec, vmem_spec),
        scratch_shapes=[
            pltpu.VMEM((FL * 2 * NBLK, BLK), F32),
            pltpu.VMEM((KP, NP), F32),
            pltpu.VMEM((2, TL), F32),
            pltpu.VMEM((FD, 2, TL), F32),
            pltpu.VMEM((16, 128), F32),
            pltpu.VMEM((2, 64, FD * 64), BF16),
            pltpu.VMEM((2, FD * KP, FD * KP), BF16),
            *[pltpu.VMEM((FD * KP, width), F32) for _, width in CHUNKS],
            *[pltpu.VMEM((FD, TL, width), F32) for _, width in CHUNKS],
            pltpu.VMEM((2, 16 * NHALF, BLK), F32),
            pltpu.VMEM((16 * NHALF, BLK), F32),
            pltpu.VMEM((16 * NHALF, BLK), F32),
            pltpu.VMEM((FD, 2 * NHALF, BLK), F32),
            pltpu.VMEM((MD * SLOTS, BLK), F32),
            pltpu.VMEM((MD * SLOTS, BLK), F32),
            pltpu.VMEM((GROUPS, MD * SLOTS), BF16),
            pltpu.VMEM((MD, 2 * SLOTS, BLK), F32),
            pltpu.VMEM((MD, 2 * SLOTS, BLK), F32),
            pltpu.VMEM((GROUPS * BLK, BLK), F32),
            pltpu.VMEM((GROUPS * BLK, 2 * BLK), BF16),
            pltpu.VMEM((4, 512, EXT), BF16),
            pltpu.VMEM((2 * ROWS, 128), F32),
            pltpu.VMEM((4 * ROWS, 128), F32),
            pltpu.VMEM((4, ROWS), jnp.int32),
            pltpu.VMEM((1, 128), jnp.int32),
            pltpu.SMEM((1,), jnp.int32),
            pltpu.VMEM((2, HALO, 128), F32),
            pltpu.VMEM((2, HALO, 128), F32),
            pltpu.VMEM((2, HALO, 128), F32),
            pltpu.VMEM((HALO, 128), F32),
            pltpu.VMEM((HALO, 128), F32),
            pltpu.VMEM((EXT, 256), BF16),
            pltpu.VMEM((ROWS, 128), F32),
            pltpu.VMEM((ROWS, 128), F32),
            pltpu.VMEM((2, 4 * GROUPS, BLK), F32),
            pltpu.VMEM((4 * GROUPS, BLK), F32),
            sem((16,)),
            sem((FD,)), sem((FD,)),
            sem((len(CHUNKS), FD)), sem((len(CHUNKS), FD)),
            sem((FD,)), sem((FD,)),
            sem((MD,)), sem((MD,)),
            sem((MD,)), sem((MD,)),
            sem((6,)), sem((6,)),
            sem((len(CHUNKS), FD)), sem((len(CHUNKS), FD)),
            pltpu.SemaphoreType.REGULAR,
        ],
        compiler_params=pltpu.CompilerParams(
            collective_id=0, has_side_effects=True, vmem_limit_bytes=62 * 1024 * 1024
        ),
        name="p2o_wave",
    )(
        spec, time_weights, interp_weights.reshape(GROUPS * BLK, BLK), group_block.reshape(1, GROUPS),
        group_count, ws, neighbors, cp, jnp.asarray(basis), jnp.asarray(own),
    )
    series, state = pl.pallas_call(
        write_out,
        out_shape=(jax.ShapeDtypeStruct((TL, NP), F32), jax.ShapeDtypeStruct((2 * ROWS, 128), F32)),
        in_specs=[pl.BlockSpec(memory_space=pltpu.VMEM)] * 2,
        out_specs=(hbm_spec, hbm_spec),
        scratch_shapes=[sem((2,))],
        name="write_out",
    )(pltpu.with_memory_space_constraint(series, pltpu.VMEM), pltpu.with_memory_space_constraint(state, pltpu.VMEM))
    new_state = state.reshape(ROWS, 2, 128).transpose(1, 0, 2).reshape(1, 2, ROWS * 128)
    return series, new_state


def solution(mesh):
    in_specs = (
        P(None, "freq", "mesh"),
        P(None, "freq"),
        P("mesh", None, None),
        P("mesh"),
        P("mesh"),
        P("freq", None, "mesh"),
        P(None, "mesh"),
        P(None, "mesh"),
    )
    out_specs = (P("freq", "mesh"), P("freq", None, "mesh"))
    return jax.shard_map(local_step, mesh=mesh, in_specs=in_specs, out_specs=out_specs, check_vma=False)
```

```python
import functools
import math

import jax
import jax.numpy as jnp
import numpy as np
from jax import lax
from jax.experimental import pallas as pl
from jax.experimental.pallas import tpu as pltpu
from jax.sharding import PartitionSpec as P

MESH = pl.DeviceIdType.MESH
F32 = jnp.float32
BF16 = jnp.bfloat16

NF = 216
NT = 432
FD = 8
MD = 16
FL = NF // FD
TL = NT // FD
KP = 56
NP = 4096
COLS = NP // FD
CHUNKS = ((0, 256), (256, 128), (384, 128))
EARLY = 2
BLK = 128
NBLK = NP // BLK
NHALF = NBLK // 2
GROUPS = 128
ROWS = 512
HALO = 32
EXT = 640
SLOTS = 8


def split_bf16(x):
    hi = x.astype(BF16)
    lo = (x - hi.astype(F32)).astype(BF16)
    return hi, lo


def host_split(x):
    hi = np.asarray(x, np.float32).astype(jnp.bfloat16)
    lo = (x - hi.astype(np.float64)).astype(jnp.bfloat16)
    return hi, lo


def host_basis():
    t = np.arange(NT)[:, None]
    k = np.arange(NF)[None, :]
    angle = (t * k % NT) * (2.0 * math.pi / NT)
    scale = np.where(k == 0, 1.0, 2.0) / NT
    full = np.zeros((FD, KP, FD, KP))
    full[:, :TL, :, :FL] = (np.cos(angle) * scale).reshape(FD, TL, FD, FL)
    full[:, :TL, :, FL : 2 * FL] = (-np.sin(angle) * scale).reshape(FD, TL, FD, FL)
    basis = np.stack(host_split(full.reshape(FD * KP, FD * KP)))
    own = np.zeros((FD, 64, FD, 64))
    own[:, :KP, :, :KP] = full.transpose(2, 1, 0, 3)
    own = own.reshape(FD, 64, FD * 64)
    return basis, np.stack(host_split(own), axis=1)


def dot(a, b):
    return jnp.dot(a, b, preferred_element_type=F32)


def dot_t(a, b):
    return lax.dot_general(a, b, (((1,), (1,)), ((), ())), preferred_element_type=F32)


def kernel(
    spec_h, tw_h, w_h, gb_h, gc_h, ws_h, nb_h, cp_h, basis_h, own_h,
    series_o, state_o,
    xs, xp, tws, twr, twf, cb, basis, r0, r1, r2, s20, s21, s22, pb, pr, ps, ra, rs, rq, pt, gs, gr, wf, whl, oh, ws, cp, nb, gb, gc,
    hs, hcur, hb1, hpush, hps, sb, base1, base2, lh, ee,
    lsem, tw_s, tw_r, x_s, x_r, a_s, a_r, q_s, q_r, g_s, g_r, h_s, h_r, y_s, y_r, mesh_sem,
):
    r = (r0, r1, r2)
    s2 = (s20, s21, s22)
    f = lax.axis_index("freq")
    m = lax.axis_index("mesh")

    def fdev(d):
        return (lax.rem(f + d, FD), m)

    def mdev(d):
        return (f, lax.rem(m + d, MD))

    def remote(src, dst, ssem, rsem, dev):
        return pltpu.make_async_remote_copy(
            src_ref=src, dst_ref=dst, send_sem=ssem, recv_sem=rsem, device_id=dev, device_id_type=MESH
        )

    bar = pltpu.get_barrier_semaphore()

    def tell(sem, dev):
        pl.semaphore_signal(sem, inc=1, device_id=dev, device_id_type=MESH)

    for d in range(1, FD):
        tell(bar, fdev(d))
    for d in range(1, MD):
        pl.when(m + d < MD)(functools.partial(tell, bar, mdev(d)))

    loads = [
        (spec_h, xs.at[0 : FL * 2 * NBLK]), (tw_h, tws), (own_h.at[f], cb), (nb_h, nb), (gb_h, gb), (gc_h, gc),
        (ws_h, ws), (cp_h, cp), (basis_h, basis), (w_h, wf),
    ]
    local = [pltpu.make_async_copy(s, d, lsem.at[i]) for i, (s, d) in enumerate(loads)]
    for c in local[:7]:
        c.start()

    twf[...] = jnp.zeros_like(twf)
    xp[KP - 8 :, :] = jnp.zeros((8, NP), F32)
    sb[ROWS:, :] = jnp.zeros((EXT - ROWS, 256), BF16)
    local[0].wait()
    for ct in range(NBLK):
        for part in range(2):
            xp[FL * part : FL * (part + 1), BLK * ct : BLK * (ct + 1)] = xs[pl.ds(2 * ct + part, FL, stride=2 * NBLK), :]
    local[1].wait()
    local[6].wait()
    hs[0] = ws[pl.ds(1, HALO, stride=2), :]
    hs[1] = ws[pl.ds(2 * (ROWS - HALO) + 1, HALO, stride=2), :]

    pl.semaphore_wait(bar, FD - 1 + m)

    tw_c = [remote(tws, twr.at[f], tw_s.at[d], tw_r.at[d], fdev(d)) for d in range(1, FD)]
    for c in tw_c:
        c.start()

    def cols_of(dev, h):
        first, width = CHUNKS[h]
        return pl.ds(pl.multiple_of(dev * COLS + first, 128), width)

    def x_copy(h, d):
        to = lax.rem(f + d, FD)
        rows = pl.ds(pl.multiple_of(f * KP, 8), KP)
        return remote(xp.at[:, cols_of(to, h)], r[h].at[rows], x_s.at[h, d], x_r.at[h, d], (to, m))

    x_c = [[x_copy(h, d) for d in range(1, FD)] for h in range(len(CHUNKS))]
    for h in range(EARLY):
        for c in x_c[h]:
            c.start()
    for d in range(1, MD):
        pl.when(m >= d)(functools.partial(tell, mesh_sem, mdev(MD - d)))
    for c in local[7:]:
        c.start()
    own_x = [
        pltpu.make_async_copy(
            xp.at[:, cols_of(f, h)], r[h].at[pl.ds(pl.multiple_of(f * KP, 8), KP)], lsem.at[10 + h]
        )
        for h in range(len(CHUNKS))
    ]
    for c in own_x:
        c.start()

    local[4].wait()
    local[5].wait()
    index = lax.broadcasted_iota(jnp.int32, (1, GROUPS), 1)
    live = index < gc[0]
    gbv = gb[...]
    owner = jnp.where(live, lax.shift_right_logical(gbv, 5), -1).astype(F32)
    inner = (lax.bitwise_and(gbv, NBLK - 1) + 1).astype(F32)
    lane_i = lax.broadcasted_iota(jnp.int32, (128, 128), 1)
    lane = lane_i.astype(F32)
    owner_r = jnp.broadcast_to(owner, (128, 128))
    owner_c = jnp.transpose(owner_r)
    earlier = lane_i < lax.broadcasted_iota(jnp.int32, (128, 128), 0)
    rank = jnp.sum(jnp.where(jnp.logical_and(owner_r == owner_c, earlier), 1.0, 0.0), axis=1, keepdims=True)
    slot = jnp.where(owner_c >= 0.0, owner_c * SLOTS + rank, -1.0)
    place = jnp.where(slot == lane, 1.0, 0.0)
    asked = jnp.sum(jnp.transpose(place) * inner, axis=1, keepdims=True) - 1.0
    rs[...] = jnp.broadcast_to(asked, (128, 128))
    pt[...] = place.astype(BF16)

    def q_copy(d):
        to = lax.rem(m + d, MD)
        src = rs.at[pl.ds(pl.multiple_of(to * SLOTS, 8), SLOTS)]
        dst = rq.at[pl.ds(pl.multiple_of(m * SLOTS, 8), SLOTS)]
        return remote(src, dst, q_s.at[d], q_r.at[d], (f, to))

    q_c = [q_copy(d) for d in range(1, MD)]
    rq[pl.ds(pl.multiple_of(m * SLOTS, 8), SLOTS), :] = rs[pl.ds(pl.multiple_of(m * SLOTS, 8), SLOTS), :]
    up, down = mdev(1), mdev(MD - 1)
    above, below = m < MD - 1, m > 0

    def halo_pair(i, low_src, high_src, dst):
        return [
            (remote(low_src, dst.at[1], h_s.at[i], h_r.at[i], down), below, above),
            (remote(high_src, dst.at[0], h_s.at[i + 1], h_r.at[i + 1], up), above, below),
        ]

    def start_all(pairs):
        for c, sends, _ in pairs:
            pl.when(sends)(functools.partial(c.start))

    def recv_all(pairs):
        for c, _, gets in pairs:
            pl.when(gets)(c.wait_recv)

    cur_c = halo_pair(0, hs.at[0], hs.at[1], hcur)

    def enter_mesh():
        pl.when(above)(lambda: pl.semaphore_wait(mesh_sem, MD - 1 - m))
        for c in q_c:
            c.start()
        start_all(cur_c)

    pl.when(m >= MD // 2)(enter_mesh)

    local[2].wait()
    for c in tw_c:
        c.wait_recv()
    twr[f] = tws[...]
    for w in range(FD):
        twf[2 * w : 2 * w + 2, 0:TL] = twr[w]
    th, tl = split_bf16(twf[:, 0:64])
    g_all = dot(th, cb[0]) + dot(tl, cb[0]) + dot(th, cb[1])
    row_w = lax.broadcasted_iota(jnp.int32, (16, 128), 0) // 2
    lane_w = lax.broadcasted_iota(jnp.int32, (16, 128), 1) // 64
    g2 = jnp.zeros((16, 128), F32)
    for i in range(4):
        g2 = g2 + jnp.where(lane_w + 2 * i == row_w, g_all[:, 128 * i : 128 * (i + 1)], 0.0)
    g = (g2 + pltpu.roll(g2, 64, 1))[:, 0:KP]
    gh, gl = split_bf16(g)
    ghl = jnp.concatenate([gh, gl], axis=0)
    for q in range(8):
        xh, xl = split_bf16(xp[:, 512 * q : 512 * (q + 1)])
        both = dot(ghl, xh)
        part = both[0:16] + both[16:32] + dot(gh, xl)
        for b in range(4):
            pb[q // 4, pl.ds(4 * (q % 4) + b, 16, stride=NHALF), :] = part[:, 128 * b : 128 * (b + 1)]

    core = lax.rem(f, 2)
    pair_c = remote(pb.at[1 - core], pr, a_s.at[0], a_r.at[0], (f + 1 - 2 * core, m))
    pair_c.start()
    pair_c.wait_recv()
    ps[...] = pb[core] + pr[...]

    def a_copy(d):
        to = lax.rem(f + d, FD)
        src = ps.at[pl.ds(pl.multiple_of(to * 2 * NHALF, 8), 2 * NHALF)]
        return remote(src, ra.at[f], a_s.at[d], a_r.at[d], (to, m))

    a_c = [a_copy(d) for d in range(1, FD)]
    for c in a_c:
        c.start()
    for h in range(EARLY, len(CHUNKS)):
        for c in x_c[h]:
            c.start()
    ra[f] = ps[pl.ds(pl.multiple_of(f * 2 * NHALF, 8), 2 * NHALF), :]

    local[3].wait()
    nbv = nb[...]
    nbv = jnp.where(nbv >= ROWS + HALO, nbv, jnp.where(nbv < HALO, nbv + ROWS, nbv - HALO)).astype(F32)
    for n in range(4):
        for ut in range(4):
            col = jnp.transpose(jnp.broadcast_to(nbv[n : n + 1, 128 * ut : 128 * (ut + 1)], (128, 128)))
            for kt in range(EXT // 128):
                hot = jnp.where(col == lane + float(128 * kt), 1.0, 0.0).astype(BF16)
                oh[ut, 128 * n : 128 * (n + 1), 128 * kt : 128 * (kt + 1)] = hot

    local[9].wait()

    def split_w(i, carry):
        rows = pl.ds(pl.multiple_of(i * 512, 512), 512)
        hi, lo = split_bf16(wf[rows, :])
        whl[rows, 0:128] = hi
        whl[rows, 128:256] = lo
        return carry

    lax.fori_loop(0, GROUPS * BLK // 512, split_w, 0)

    pl.when(m < MD // 2)(enter_mesh)

    local[8].wait()

    def y_copy(h, d):
        to = lax.rem(f + d, FD)
        return remote(s2[h].at[to], series_o.at[:, cols_of(f, h)], y_s.at[h, d], y_r.at[h, d], (to, m))

    y_c = [[y_copy(h, d) for d in range(1, FD)] for h in range(len(CHUNKS))]
    own_y = []

    def transform(h):
        for c in x_c[h]:
            c.wait_recv()
        own_x[h].wait()
        xh, xl = split_bf16(r[h][...])
        out = dot(basis[0], xh) + dot(basis[0], xl) + dot(basis[1], xh)
        for w in range(FD):
            s2[h][w] = out[KP * w : KP * w + TL]
        for c in y_c[h]:
            c.start()
        c = pltpu.make_async_copy(
            s2[h].at[f], series_o.at[:, cols_of(f, h)], lsem.at[13 + h]
        )
        c.start()
        own_y.append(c)


    transform(0)

    for c in q_c:
        c.wait_recv()
    sel = jnp.where(rq[...] == lane, 1.0, 0.0).astype(BF16)[:, 0:NBLK]
    for c in a_c:
        c.wait_recv()
    total = [ra[c] + ra[2 + c] + ra[4 + c] + ra[6 + c] for c in range(2)]
    for s in range(2):
        rows = slice(NHALF * s, NHALF * (s + 1))
        hi, lo = split_bf16(jnp.concatenate([total[0][rows], total[1][rows]], axis=0))
        out = dot(sel, hi) + dot(sel, lo)
        for o in range(MD):
            gs[o, SLOTS * s : SLOTS * (s + 1), :] = out[SLOTS * o : SLOTS * (o + 1)]

    def g_copy(d):
        to = lax.rem(m + d, MD)
        return remote(gs.at[to], gr.at[m], g_s.at[d], g_r.at[d], (f, to))

    g_c = [g_copy(d) for d in range(1, MD)]
    for c in g_c:
        c.start()
    gr[m] = gs[m]

    for i in (7,):
        local[i].wait()

    def put_ext(lo_row, value):
        hi, lo = split_bf16(value)
        sb[lo_row : lo_row + value.shape[0], 0:128] = hi
        sb[lo_row : lo_row + value.shape[0], 128:256] = lo

    def put_halo(buf):
        put_ext(ROWS, jnp.where(m > 0, buf[0], 0.0))
        put_ext(ROWS + HALO, jnp.where(m < MD - 1, buf[1], 0.0))

    def spread(ut, v):
        e = dot(oh[ut], sb[...])
        total = jnp.zeros((128, 128), F32)
        for n in range(4):
            c = cp[pl.ds(512 * ut + n, 128, stride=4), :]
            total = total + c * (e[128 * n : 128 * (n + 1), 0:128] + e[128 * n : 128 * (n + 1), 128:256] - v)
        return total

    put_ext(0, ws[pl.ds(1, ROWS, stride=2), :])
    recv_all(cur_c)
    put_halo(hcur)
    for ut in range(4):
        cur = ws[pl.ds(256 * ut + 1, 128, stride=2), :]
        prev = ws[pl.ds(256 * ut, 128, stride=2), :]
        base1[128 * ut : 128 * (ut + 1), :] = 2.0 * cur - prev + spread(ut, cur)
    b1_c = halo_pair(2, base1.at[0:HALO], base1.at[ROWS - HALO : ROWS], hb1)
    start_all(b1_c)

    transform(1)
    transform(2)

    put_ext(0, base1[...])
    recv_all(b1_c)
    put_halo(hb1)
    for ut in range(4):
        cur = ws[pl.ds(256 * ut + 1, 128, stride=2), :]
        b1 = base1[128 * ut : 128 * (ut + 1), :]
        base2[128 * ut : 128 * (ut + 1), :] = 2.0 * b1 - cur + spread(ut, b1)

    for c in g_c:
        c.wait_recv()
    for s in range(2):
        blocks = gr[:, SLOTS * s : SLOTS * (s + 1), :].reshape(MD * SLOTS, BLK)
        hi, lo = split_bf16(blocks)
        ph = dot(pt[...], hi)
        lh[0, pl.ds(2 * s, 128, stride=4), :] = ph
        lh[1, pl.ds(2 * s, 128, stride=4), :] = ph
        lh[0, pl.ds(2 * s + 1, 128, stride=4), :] = dot(pt[...], lo)
        lh[1, pl.ds(2 * s + 1, 128, stride=4), :] = jnp.zeros((128, 128), F32)
    upper = lax.broadcasted_iota(jnp.int32, (8, 128), 0) < 4

    def interp(i, carry):
        for j in range(16):
            rows = pl.ds(pl.multiple_of(i * 128 + 8 * j, 8), 8)
            w = whl[pl.ds(pl.multiple_of(i * 4096 + 256 * j, 256), 256), :]
            left = jnp.concatenate([lh[0, rows, :], lh[1, rows, :]], axis=1).astype(BF16)
            out = dot_t(left, w)
            ee[rows, :] = jnp.where(upper, out[:, 0:128], out[:, 128:256])
        return carry

    interp(0, 0)
    hps[...] = ee[pl.ds(0, HALO, stride=4), :] + ee[pl.ds(1, HALO, stride=4), :]
    p_c = [(remote(hps, hpush, h_s.at[4], h_r.at[4], down), below, above)]
    start_all(p_c)
    for i in range(1, GROUPS // 32):
        interp(i, 0)
    push0 = ee[pl.ds(0, 128, stride=4), :] + ee[pl.ds(1, 128, stride=4), :]
    push1 = ee[pl.ds(2, 128, stride=4), :] + ee[pl.ds(3, 128, stride=4), :]

    sb[ROWS : ROWS + HALO, :] = jnp.zeros((HALO, 256), BF16)
    put_ext(0, push0)
    recv_all(p_c)
    put_ext(ROWS + HALO, jnp.where(m < MD - 1, hpush[...], 0.0))
    for ut in range(4):
        e = dot(oh[ut, :, 0:128], sb[0:128, :]) + dot(oh[ut, :, ROWS:EXT], sb[ROWS:EXT, :])
        total = jnp.zeros((128, 128), F32)
        for n in range(4):
            c = cp[pl.ds(512 * ut + n, 128, stride=4), :]
            en = e[128 * n : 128 * (n + 1), 0:128] + e[128 * n : 128 * (n + 1), 128:256]
            total = total + c * (en - push0 if ut == 0 else en)
        n1 = base1[128 * ut : 128 * (ut + 1), :]
        n2 = base2[128 * ut : 128 * (ut + 1), :] + total
        if ut == 0:
            n1 = n1 + push0
            n2 = n2 + 2.0 * push0 + push1
        state_o[pl.ds(256 * ut, 128, stride=2), :] = n1
        state_o[pl.ds(256 * ut + 1, 128, stride=2), :] = n2

    for c in [pair_c] + tw_c + sum(x_c, []) + a_c + q_c + g_c + sum(y_c, []):
        c.wait_send()
    for c, sends, _ in cur_c + b1_c + p_c:
        pl.when(sends)(c.wait_send)
    for c in sum(y_c, []):
        c.wait_recv()
    for c in own_y:
        c.wait()


def write_out(series, state, series_o, state_o, sem):
    copies = [pltpu.make_async_copy(series, series_o, sem.at[0]), pltpu.make_async_copy(state, state_o, sem.at[1])]
    for c in copies:
        c.start()
    for c in copies:
        c.wait()


def local_step(spectrum, time_weights, interp_weights, group_block, group_count, wave_state, neighbors, coupling):
    basis, own = host_basis()
    ws = wave_state.reshape(2, ROWS, 128).transpose(1, 0, 2).reshape(2 * ROWS, 128)
    cp = coupling.reshape(4, ROWS, 128).transpose(1, 0, 2).reshape(4 * ROWS, 128)
    hbm_spec = pl.BlockSpec(memory_space=pltpu.HBM)
    vmem_spec = pl.BlockSpec(memory_space=pltpu.VMEM)
    sem = pltpu.SemaphoreType.DMA
    spec = spectrum.reshape(2, FL, NBLK, BLK).transpose(1, 2, 0, 3).reshape(FL * 2 * NBLK, BLK)
    series, state = pl.pallas_call(
        kernel,
        out_shape=(pltpu.VMEM((TL, NP), F32), pltpu.VMEM((2 * ROWS, 128), F32)),
        in_specs=[hbm_spec] * 10,
        out_specs=(vmem_spec, vmem_spec),
        scratch_shapes=[
            pltpu.VMEM((32 * 2 * NBLK, BLK), F32),
            pltpu.VMEM((KP, NP), F32),
            pltpu.VMEM((2, TL), F32),
            pltpu.VMEM((FD, 2, TL), F32),
            pltpu.VMEM((16, 128), F32),
            pltpu.VMEM((2, 64, FD * 64), BF16),
            pltpu.VMEM((2, FD * KP, FD * KP), BF16),
            *[pltpu.VMEM((FD * KP, width), F32) for _, width in CHUNKS],
            *[pltpu.VMEM((FD, TL, width), F32) for _, width in CHUNKS],
            pltpu.VMEM((2, 16 * NHALF, BLK), F32),
            pltpu.VMEM((16 * NHALF, BLK), F32),
            pltpu.VMEM((16 * NHALF, BLK), F32),
            pltpu.VMEM((FD, 2 * NHALF, BLK), F32),
            pltpu.VMEM((MD * SLOTS, BLK), F32),
            pltpu.VMEM((MD * SLOTS, BLK), F32),
            pltpu.VMEM((GROUPS, MD * SLOTS), BF16),
            pltpu.VMEM((MD, 2 * SLOTS, BLK), F32),
            pltpu.VMEM((MD, 2 * SLOTS, BLK), F32),
            pltpu.VMEM((GROUPS * BLK, BLK), F32),
            pltpu.VMEM((GROUPS * BLK, 2 * BLK), BF16),
            pltpu.VMEM((4, 512, EXT), BF16),
            pltpu.VMEM((2 * ROWS, 128), F32),
            pltpu.VMEM((4 * ROWS, 128), F32),
            pltpu.VMEM((4, ROWS), jnp.int32),
            pltpu.VMEM((1, 128), jnp.int32),
            pltpu.SMEM((1,), jnp.int32),
            pltpu.VMEM((2, HALO, 128), F32),
            pltpu.VMEM((2, HALO, 128), F32),
            pltpu.VMEM((2, HALO, 128), F32),
            pltpu.VMEM((HALO, 128), F32),
            pltpu.VMEM((HALO, 128), F32),
            pltpu.VMEM((EXT, 256), BF16),
            pltpu.VMEM((ROWS, 128), F32),
            pltpu.VMEM((ROWS, 128), F32),
            pltpu.VMEM((2, 4 * GROUPS, BLK), F32),
            pltpu.VMEM((4 * GROUPS, BLK), F32),
            sem((16,)),
            sem((FD,)), sem((FD,)),
            sem((len(CHUNKS), FD)), sem((len(CHUNKS), FD)),
            sem((FD,)), sem((FD,)),
            sem((MD,)), sem((MD,)),
            sem((MD,)), sem((MD,)),
            sem((6,)), sem((6,)),
            sem((len(CHUNKS), FD)), sem((len(CHUNKS), FD)),
            pltpu.SemaphoreType.REGULAR,
        ],
        compiler_params=pltpu.CompilerParams(
            collective_id=0, has_side_effects=True, vmem_limit_bytes=62 * 1024 * 1024
        ),
        name="p2o_wave",
    )(
        spec, time_weights, interp_weights.reshape(GROUPS * BLK, BLK), group_block.reshape(1, GROUPS),
        group_count, ws, neighbors, cp, jnp.asarray(basis), jnp.asarray(own),
    )
    series, state = pl.pallas_call(
        write_out,
        out_shape=(jax.ShapeDtypeStruct((TL, NP), F32), jax.ShapeDtypeStruct((2 * ROWS, 128), F32)),
        in_specs=[pl.BlockSpec(memory_space=pltpu.VMEM)] * 2,
        out_specs=(hbm_spec, hbm_spec),
        scratch_shapes=[sem((2,))],
        name="write_out",
    )(pltpu.with_memory_space_constraint(series, pltpu.VMEM), pltpu.with_memory_space_constraint(state, pltpu.VMEM))
    new_state = state.reshape(ROWS, 2, 128).transpose(1, 0, 2).reshape(1, 2, ROWS * 128)
    return series, new_state


def solution(mesh):
    in_specs = (
        P(None, "freq", "mesh"),
        P(None, "freq"),
        P("mesh", None, None),
        P("mesh"),
        P("mesh"),
        P("freq", None, "mesh"),
        P(None, "mesh"),
        P(None, "mesh"),
    )
    out_specs = (P("freq", "mesh"), P("freq", None, "mesh"))
    return jax.shard_map(local_step, mesh=mesh, in_specs=in_specs, out_specs=out_specs, check_vma=False)
```
